8 devices in a mesh: dp: 1 (over z), ep: 8 (over y, x, core).
Axes of the slice: x: 2, y: 2, z: 1, core: 2. Of those that a mesh axis runs over, the one named last changes fastest.
Arguments:
- x_rows: bfloat16 [8192, 768], P(('dp', 'ep'))
- sel_idx: int32 [64, 256], P(('dp', 'ep'))
- gate_w: float32 [64, 256], P(('dp', 'ep'))
- w_up: bfloat16 [64, 768, 3072], P('ep')
- w_down: bfloat16 [64, 3072, 768], P('ep')
Outputs:
- output: bfloat16 [8192, 768], P(('dp', 'ep'))
All inputs are finite; a program needn't handle non-finite values.
Results may differ from the reference program's by a relative error of at most 0.00676407.
Values are sent between devices in bfloat16 or wider.
A program may use at most 1 GiB of HBM per device.

```python
import jax
import jax.numpy as jnp
from jax import lax

D_MODEL = 768
D_FF = 3072
EXPERTS = 64
GROUP_SIZE = 8
TOKENS = 8192
CAPACITY = 256

TOK_LOC = TOKENS // GROUP_SIZE
EXP_LOC = EXPERTS // GROUP_SIZE
PER_SOURCE = CAPACITY // GROUP_SIZE


def draw_selection(sel_key):
    key_order, key_hot, key_rank, key_delta, key_rows, key_cols = jax.random.split(sel_key, 6)
    dev_order = jax.random.permutation(key_order, GROUP_SIZE)
    hot_owner = dev_order[jax.random.randint(key_hot, (GROUP_SIZE,), 0, max(1, GROUP_SIZE // 4))]
    hot_expert = jnp.repeat(hot_owner, EXP_LOC)
    rank_keys = jax.random.randint(key_rank, (EXPERTS, GROUP_SIZE), 0, 1048576)
    rank_keys = jnp.where(jnp.arange(GROUP_SIZE)[None, :] == hot_expert[:, None], -1, rank_keys)
    src_order = jnp.argsort(rank_keys, axis=1, stable=True)
    delta_rows = jax.random.randint(key_delta, (EXPERTS, (GROUP_SIZE - 2) // 2), 0, PER_SOURCE + 1)
    paired = jnp.stack([PER_SOURCE + delta_rows, PER_SOURCE - delta_rows], axis=2).reshape(EXPERTS, GROUP_SIZE - 2)
    count_by_pos = jnp.concatenate([jnp.full((EXPERTS, 1), 2 * PER_SOURCE, jnp.int32), paired.astype(jnp.int32), jnp.zeros((EXPERTS, 1), jnp.int32)], axis=1)
    count_dev = jnp.take_along_axis(count_by_pos, jnp.argsort(src_order, axis=1), axis=1)
    row_ends = jnp.cumsum(count_dev, axis=1)
    row_starts = row_ends - count_dev
    slot_ids = jnp.arange(CAPACITY)
    source = jnp.sum((row_ends[:, None, :] <= slot_ids[None, :, None]).astype(jnp.int32), axis=2)
    rank_in = slot_ids[None, :] - jnp.take_along_axis(row_starts, source, axis=1)
    row_perm = jnp.argsort(jax.random.bits(key_rows, (EXPERTS, GROUP_SIZE, TOK_LOC)), axis=2).reshape(EXPERTS, TOKENS)
    picked = jnp.take_along_axis(row_perm, source * TOK_LOC + rank_in, axis=1)
    tokens = source * TOK_LOC + picked
    col_perm = jnp.argsort(jax.random.bits(key_cols, (EXPERTS, CAPACITY)), axis=1)
    return jnp.take_along_axis(tokens, col_perm, axis=1).astype(jnp.int32)


def setup_inputs(seed: int = 0, part: int = 0) -> dict:
    base_key = jax.random.key(seed)
    part_key = jax.random.fold_in(base_key, part)
    key_x, key_sel, key_gate = jax.random.split(part_key, 3)
    key_up, key_down = jax.random.split(jax.random.key(seed + 1), 2)
    up_scale = D_MODEL ** -0.5
    down_scale = 1.5 * D_FF ** -0.5
    x_rows = jax.random.normal(key_x, (TOKENS, D_MODEL), jnp.float32).astype(jnp.bfloat16)
    sel_idx = draw_selection(key_sel)
    gate_w = jax.random.uniform(key_gate, (EXPERTS, CAPACITY), jnp.float32, 0.25, 1.25)
    w_up = (jax.random.normal(key_up, (EXPERTS, D_MODEL, D_FF), jnp.float32) * up_scale).astype(jnp.bfloat16)
    w_down = (jax.random.normal(key_down, (EXPERTS, D_FF, D_MODEL), jnp.float32) * down_scale).astype(jnp.bfloat16)
    return {"x_rows": x_rows, "sel_idx": sel_idx, "gate_w": gate_w, "w_up": w_up, "w_down": w_down}


def reference(x_rows, sel_idx, gate_w, w_up, w_down):
    def one_expert(expert_args):
        sel_row, gate_row, up_mat, down_mat = expert_args
        chosen = jnp.take(x_rows, sel_row, axis=0)
        hidden = jax.nn.gelu(jnp.dot(chosen, up_mat, preferred_element_type=jnp.float32), approximate=True).astype(jnp.bfloat16)
        out_rows = jnp.dot(hidden, down_mat, preferred_element_type=jnp.float32)
        return (out_rows * gate_row[:, None]).astype(jnp.bfloat16)

    contrib = lax.map(one_expert, (sel_idx, gate_w, w_up, w_down))
    summed = jax.ops.segment_sum(contrib.reshape(EXPERTS * CAPACITY, D_MODEL).astype(jnp.float32), sel_idx.reshape(EXPERTS * CAPACITY), num_segments=TOKENS)
    return (x_rows.astype(jnp.float32) + summed).astype(jnp.bfloat16)
```

```python
import functools

import jax
import jax.numpy as jnp
from jax import lax
from jax.experimental import pallas as pl
from jax.experimental.pallas import tpu as pltpu
from jax.sharding import PartitionSpec as P

F32 = jnp.float32
BF16 = jnp.bfloat16
MESH = pl.DeviceIdType.MESH

NDEV = 8
CHUNKS = 8
LAG = 2


def _gelu(z):
    return 0.5 * z * (1.0 + jnp.tanh(0.7978845608028654 * (z + 0.044715 * (z * z * z))))


def _iota(shape, dim):
    return lax.broadcasted_iota(jnp.int32, shape, dim)


def _onehot(cond):
    return jnp.where(cond, 1.0, 0.0).astype(BF16)


def kernel(
    slots,
    x_ref, sel_ref, gate_ref, up_ref, down_ref,
    y_ref,
    xall, wup, wdn, send, ret, acc, pk, hid, pmat, yacc,
    sel_t, gate_t, code_s, rt_send, rt_recv, rowtab,
    own_sem, wup_sem, wdn_sem, agx_sem, agy_sem, ags_sem, agr_sem,
    rts_sem, rtr_sem, snd_sem, rcv_sem, loc_sem,
):
    n_exp, cap = sel_ref.shape
    tok, width = x_ref.shape
    ff = up_ref.shape[2]
    nslot = NDEV * slots
    me = lax.axis_index("ep")
    core = me % 2
    sib = me + 1 - 2 * core
    xx = (me // 2) % 2
    yy = me // 4
    dx = 2 - 4 * xx
    dy = 4 - 8 * yy
    xn, yn, dg = me + dx, me + dy, me + dx + dy
    peers = (dg, sib + dx + dy, xn, sib + dx, yn, sib + dy, sib)
    ch = tok // CHUNKS
    half = CHUNKS // 2

    def remote(src, dst, ssem, rsem, dev):
        return pltpu.make_async_remote_copy(
            src_ref=src, dst_ref=dst, send_sem=ssem, recv_sem=rsem, device_id={"ep": dev}, device_id_type=MESH
        )

    def up_copy(e):
        return pltpu.make_async_copy(up_ref.at[e], wup.at[e % 2], wup_sem.at[e % 2])

    def down_copy(e):
        return pltpu.make_async_copy(down_ref.at[e], wdn.at[e % 2], wdn_sem.at[e % 2])

    own_copy = pltpu.make_async_copy(x_ref, xall.at[me], own_sem)
    own_copy.start()

    barrier = pltpu.get_barrier_semaphore()
    for dev in peers:
        pl.semaphore_signal(barrier, inc=1, device_id={"ep": dev}, device_id_type=MESH)
    pl.semaphore_wait(barrier, NDEV - 1)
    own_copy.wait()

    def piece(owner, c):
        return xall.at[owner, pl.ds(c * ch, ch), :]

    def ag(owner, c, ssem, dev):
        return remote(piece(owner, c), piece(owner, c), ssem, agr_sem.at[owner, c], dev)

    sends = []

    def go(copy):
        copy.start()
        sends.append(copy)

    nx, ny, ns = 0, 0, 0
    for i in range(CHUNKS):
        go(ag(me, i, agx_sem.at[nx], xn))
        go(ag(me, (i + half) % CHUNKS, agy_sem.at[ny], yn))
        go(ag(me, i, ags_sem.at[ns], sib))
        nx, ny, ns = nx + 1, ny + 1, ns + 1

    for e in range(2):
        up_copy(e).start()
        down_copy(e).start()

    sel_t[...] = jnp.transpose(sel_ref[...].astype(F32))
    gate_t[...] = jnp.transpose(gate_ref[...])
    upper = _onehot(_iota((cap, cap), 0) < _iota((cap, cap), 1))
    for e in range(n_exp):
        sel_row = sel_ref[pl.ds(e, 1), :]
        owner = lax.shift_right_logical(sel_row, 10)
        local = jnp.bitwise_and(sel_row, 1023)
        mine = jnp.broadcast_to(owner, (16, cap)) == _iota((16, cap), 0)
        cum = jnp.dot(_onehot(mine), upper, preferred_element_type=F32)
        rank = jnp.sum(jnp.where(mine, cum, 0.0), axis=0, keepdims=True)
        owner_f = owner.astype(F32)
        code_s[pl.ds(e, 1), :] = owner_f * slots + rank
        tcode = (owner_f * 128 + rank).astype(jnp.int32) + core * slots
        q = _onehot(jnp.broadcast_to(tcode, (NDEV * 128, cap)) == _iota((NDEV * 128, cap), 0))
        hi = lax.shift_right_logical(local, 5).astype(F32)
        lo = jnp.bitwise_and(local, 31).astype(F32)
        rows = _iota((16, cap), 0)
        lhs = jnp.where(rows == 0, hi, jnp.where(rows == 1, lo, jnp.where(rows == 2, 1.0, 0.0))).astype(BF16)
        t = lax.dot_general(lhs, q, (((1,), (1,)), ((), ())), preferred_element_type=F32)
        tab = t[0:1] * 32.0 + t[1:2] + t[2:3]
        for g in range(NDEV):
            rt_send[g, pl.ds(e, 1), :] = tab[:, g * 128 : (g + 1) * 128]
    rt_recv[me] = rt_send[me]
    for k, dev in enumerate(peers):
        go(remote(rt_send.at[dev], rt_recv.at[me], rts_sem.at[k], rtr_sem.at[me], dev))

    for i in range(CHUNKS):
        cy = (i + half) % CHUNKS
        ag(xn, i, agx_sem.at[0], xn).wait_recv()
        ag(yn, cy, agy_sem.at[0], yn).wait_recv()
        if i < half:
            go(ag(xn, i, agy_sem.at[ny], yn))
            go(ag(yn, cy, agx_sem.at[nx], xn))
            nx, ny = nx + 1, ny + 1
        go(ag(xn, i, ags_sem.at[ns], sib))
        go(ag(yn, cy, ags_sem.at[ns + 1], sib))
        ns += 2
    for i in range(half):
        ag(dg, i, agy_sem.at[0], yn).wait_recv()
        ag(dg, i + half, agx_sem.at[0], xn).wait_recv()
        go(ag(dg, i, ags_sem.at[ns], sib))
        go(ag(dg, i + half, ags_sem.at[ns + 1], sib))
        ns += 2
    for dev in (sib, sib + dx, sib + dy, sib + dx + dy):
        for i in range(CHUNKS):
            ag(dev, i, ags_sem.at[0], sib).wait_recv()

    for k, dev in enumerate(peers):
        remote(rt_send.at[dev], rt_recv.at[dev], rts_sem.at[k], rtr_sem.at[dev], dev).wait_recv()
    for p in range(NDEV // 2):
        rowtab[:, p * 128 : (p + 1) * 128] = rt_recv[2 * p] + rt_recv[2 * p + 1] - 1.0
    yacc[...] = xall[me].astype(F32)

    def ret_copy(e, k, dev, src_dev):
        return remote(
            send.at[e, pl.ds(dev * slots, slots), :], ret.at[e, src_dev], snd_sem.at[e, k], rcv_sem.at[e, src_dev], dev
        )

    def loc_copy(e):
        return pltpu.make_async_copy(send.at[e, pl.ds(me * slots, slots), :], ret.at[e, me], loc_sem.at[e])

    def produce(e):
        lane8 = _iota((cap, n_exp), 1) == e
        selc = jnp.sum(jnp.where(lane8, sel_t[...], 0.0), axis=1, keepdims=True).astype(jnp.int32)
        gatec = jnp.sum(jnp.where(lane8, gate_t[...], 0.0), axis=1, keepdims=True)
        acc[...] = jnp.zeros_like(acc)

        def gather(b, carry):
            oh = _onehot(jnp.broadcast_to(selc - b * tok, (cap, tok)) == _iota((cap, tok), 1))
            acc[...] += jnp.dot(oh, xall[b], preferred_element_type=F32)
            return carry

        lax.fori_loop(0, NDEV, gather, 0)
        pk[...] = acc[...].astype(BF16)
        code = code_s[pl.ds(e, 1), :].astype(jnp.int32)
        pmat[...] = _onehot(jnp.broadcast_to(code, (nslot, cap)) == _iota((nslot, cap), 0))

        up_copy(e).wait()
        tile = 512

        def up(j, carry):
            cols = pl.ds(pl.multiple_of(j * tile, tile), tile)
            z = jnp.dot(pk[...], wup[e % 2, :, cols], preferred_element_type=F32)
            hid[:, cols] = _gelu(z).astype(BF16)
            return carry

        lax.fori_loop(0, ff // tile, up, 0)

        @pl.when(e + 2 < n_exp)
        def _():
            up_copy(e + 2).start()

        down_copy(e).wait()

        def down(j, carry):
            cols = pl.ds(pl.multiple_of(j * 256, 256), 256)
            o = jnp.dot(hid[...], wdn[e % 2, :, cols], preferred_element_type=F32)
            contrib = (o * gatec).astype(BF16)
            send[e, :, cols] = jnp.dot(pmat[...], contrib, preferred_element_type=F32).astype(BF16)
            return carry

        lax.fori_loop(0, width // 256, down, 0)

        @pl.when(e + 2 < n_exp)
        def _():
            down_copy(e + 2).start()

        for k, dev in enumerate(peers):
            ret_copy(e, k, dev, me).start()
        loc_copy(e).start()

    def combine(e):
        loc_copy(e).wait()
        for k, dev in enumerate(peers):
            ret_copy(e, k, dev, dev).wait_recv()
        row = rowtab[pl.ds(e, 1), :].astype(jnp.int32)
        tile = 256

        def add(j, carry):
            rows = pl.ds(pl.multiple_of(j * tile, tile), tile)
            s = _onehot(jnp.broadcast_to(row, (tile, nslot)) == _iota((tile, nslot), 0) + j * tile)
            yacc[rows, :] += jnp.dot(s, ret[e].reshape(nslot, width), preferred_element_type=F32)
            return carry

        lax.fori_loop(0, tok // tile, add, 0)

    def step(e, carry):
        produce(e)

        @pl.when(e >= LAG)
        def _():
            combine(e - LAG)

        return carry

    lax.fori_loop(0, n_exp, step, 0)

    def rest(e, carry):
        combine(e)
        return carry

    lax.fori_loop(n_exp - LAG, n_exp, rest, 0)
    y_ref[...] = yacc[...].astype(BF16)

    for copy in sends:
        copy.wait_send()

    def drain(e, carry):
        for k, dev in enumerate(peers):
            ret_copy(e, k, dev, me).wait_send()
        return carry

    lax.fori_loop(0, n_exp, drain, 0)


def solution(mesh):
    def local_layer(x_loc, sel_loc, gate_loc, up_loc, down_loc):
        tok, width = x_loc.shape
        n_exp, cap = sel_loc.shape
        ff = up_loc.shape[2]
        slots = 2 * cap // NDEV
        nslot = NDEV * slots
        dma = pltpu.SemaphoreType.DMA
        vmem = pl.BlockSpec(memory_space=pltpu.VMEM)
        hbm = pl.BlockSpec(memory_space=pl.ANY)
        return pl.pallas_call(
            functools.partial(kernel, slots),
            out_shape=jax.ShapeDtypeStruct((tok, width), BF16),
            in_specs=[hbm, vmem, vmem, hbm, hbm],
            out_specs=vmem,
            scratch_shapes=[
                pltpu.VMEM((NDEV, tok, width), BF16),
                pltpu.VMEM((2, width, ff), BF16),
                pltpu.VMEM((2, ff, width), BF16),
                pltpu.VMEM((n_exp, nslot, width), BF16),
                pltpu.VMEM((n_exp, NDEV, slots, width), BF16),
                pltpu.VMEM((cap, width), F32),
                pltpu.VMEM((cap, width), BF16),
                pltpu.VMEM((cap, ff), BF16),
                pltpu.VMEM((nslot, cap), BF16),
                pltpu.VMEM((tok, width), F32),
                pltpu.VMEM((cap, n_exp), F32),
                pltpu.VMEM((cap, n_exp), F32),
                pltpu.VMEM((n_exp, cap), F32),
                pltpu.VMEM((NDEV, n_exp, 128), F32),
                pltpu.VMEM((NDEV, n_exp, 128), F32),
                pltpu.VMEM((n_exp, nslot), F32),
                dma,
                dma((2,)),
                dma((2,)),
                dma((CHUNKS + CHUNKS // 2,)),
                dma((CHUNKS + CHUNKS // 2,)),
                dma((4 * CHUNKS,)),
                dma((NDEV, CHUNKS)),
                dma((NDEV - 1,)),
                dma((NDEV,)),
                dma((n_exp, NDEV - 1)),
                dma((n_exp, NDEV)),
                dma((n_exp,)),
            ],
            compiler_params=pltpu.CompilerParams(
                collective_id=0, has_side_effects=True, vmem_limit_bytes=67_000_000
            ),
            name="moe",
        )(x_loc, sel_loc, gate_loc, up_loc, down_loc)

    row_spec = P(("dp", "ep"), None)
    weight_spec = P("ep", None, None)
    return jax.shard_map(
        local_layer,
        mesh=mesh,
        in_specs=(row_spec, row_spec, row_spec, weight_spec, weight_spec),
        out_specs=row_spec,
        check_vma=False,
    )
```

```python
import functools

import jax
import jax.numpy as jnp
from jax import lax
from jax.experimental import pallas as pl
from jax.experimental.pallas import tpu as pltpu
from jax.sharding import PartitionSpec as P

F32 = jnp.float32
BF16 = jnp.bfloat16
MESH = pl.DeviceIdType.MESH

NDEV = 8
CHUNKS = 8
LAG = 2


def _gelu(z):
    return 0.5 * z * (1.0 + jnp.tanh(0.7978845608028654 * (z + 0.044715 * (z * z * z))))


def _iota(shape, dim):
    return lax.broadcasted_iota(jnp.int32, shape, dim)


def _onehot(cond):
    return jnp.where(cond, 1.0, 0.0).astype(BF16)


def kernel(
    slots,
    x_ref, sel_ref, gate_ref, up_ref, down_ref,
    y_ref,
    xall, wup, wdn, send, ret, pk, hid, pmat, yacc,
    sel_b, gate_b, code_s, rt_send, rt_recv, rowtab,
    own_sem, wup_sem, wdn_sem, agx_sem, agy_sem, ags_sem, agr_sem,
    rts_sem, rtr_sem, snd_sem, rcv_sem, loc_sem,
):
    n_exp, cap = sel_ref.shape
    tok, width = x_ref.shape
    ff = up_ref.shape[2]
    nslot = NDEV * slots
    me = lax.axis_index("ep")
    core = me % 2
    sib = me + 1 - 2 * core
    xx = (me // 2) % 2
    yy = me // 4
    dx = 2 - 4 * xx
    dy = 4 - 8 * yy
    xn, yn, dg = me + dx, me + dy, me + dx + dy
    peers = (dg, sib + dx + dy, xn, sib + dx, yn, sib + dy, sib)
    ch = tok // CHUNKS
    half = CHUNKS // 2
    yorder = [*range(CHUNKS - 1, half - 1, -1), *range(half)]

    def remote(src, dst, ssem, rsem, dev):
        return pltpu.make_async_remote_copy(
            src_ref=src, dst_ref=dst, send_sem=ssem, recv_sem=rsem, device_id={"ep": dev}, device_id_type=MESH
        )

    def up_copy(e):
        return pltpu.make_async_copy(up_ref.at[e], wup.at[e % 2], wup_sem.at[e % 2])

    def down_copy(e):
        return pltpu.make_async_copy(down_ref.at[e], wdn.at[e % 2], wdn_sem.at[e % 2])

    own_copy = pltpu.make_async_copy(x_ref, xall.at[me], own_sem)
    own_copy.start()

    barrier = pltpu.get_barrier_semaphore()
    for dev in peers:
        pl.semaphore_signal(barrier, inc=1, device_id={"ep": dev}, device_id_type=MESH)
    pl.semaphore_wait(barrier, NDEV - 1)
    own_copy.wait()

    def piece(owner, c):
        return xall.at[owner, pl.ds(c * ch, ch), :]

    def ag(owner, c, ssem, dev):
        return remote(piece(owner, c), piece(owner, c), ssem, agr_sem.at[owner, c], dev)

    sends = []

    def go(copy):
        copy.start()
        sends.append(copy)

    nx, ny, ns = 0, 0, 0
    for i in range(CHUNKS):
        go(ag(me, i, agx_sem.at[nx], xn))
        go(ag(me, yorder[i], agy_sem.at[ny], yn))
        go(ag(me, i, ags_sem.at[ns], sib))
        nx, ny, ns = nx + 1, ny + 1, ns + 1

    for e in range(2):
        up_copy(e).start()
        down_copy(e).start()

    sel_cols = jnp.transpose(sel_ref[...].astype(F32)).astype(jnp.int32)
    gate_cols = jnp.transpose(gate_ref[...])
    for e in range(n_exp):
        sel_b[e * cap : (e + 1) * cap, :] = jnp.broadcast_to(sel_cols[:, e : e + 1], (cap, 128))
        gate_b[e * cap : (e + 1) * cap, :] = jnp.broadcast_to(gate_cols[:, e : e + 1], (cap, 128))
    upper = _onehot(_iota((cap, cap), 0) < _iota((cap, cap), 1))
    for e in range(n_exp):
        sel_row = sel_ref[pl.ds(e, 1), :]
        owner = lax.shift_right_logical(sel_row, 10)
        local = jnp.bitwise_and(sel_row, 1023)
        mine = jnp.broadcast_to(owner, (16, cap)) == _iota((16, cap), 0)
        cum = jnp.dot(_onehot(mine), upper, preferred_element_type=F32)
        rank = jnp.sum(jnp.where(mine, cum, 0.0), axis=0, keepdims=True)
        owner_f = owner.astype(F32)
        code_s[pl.ds(e, 1), :] = owner_f * slots + rank
        tcode = (owner_f * 128 + rank).astype(jnp.int32) + core * slots
        q = _onehot(jnp.broadcast_to(tcode, (NDEV * 128, cap)) == _iota((NDEV * 128, cap), 0))
        hi = lax.shift_right_logical(local, 5).astype(F32)
        lo = jnp.bitwise_and(local, 31).astype(F32)
        rows = _iota((16, cap), 0)
        lhs = jnp.where(rows == 0, hi, jnp.where(rows == 1, lo, jnp.where(rows == 2, 1.0, 0.0))).astype(BF16)
        t = lax.dot_general(lhs, q, (((1,), (1,)), ((), ())), preferred_element_type=F32)
        tab = t[0:1] * 32.0 + t[1:2] + t[2:3]
        for g in range(NDEV):
            rt_send[g, pl.ds(e, 1), :] = tab[:, g * 128 : (g + 1) * 128]
    rt_recv[me] = rt_send[me]
    for k, dev in enumerate(peers):
        go(remote(rt_send.at[dev], rt_recv.at[me], rts_sem.at[k], rtr_sem.at[me], dev))

    def picks(rows, owner, first, depth):
        n = rows.size
        rel = sel_b[rows, :] - (owner * tok + first)
        lane = _iota((n, 128), 1)
        hot = jnp.concatenate([_onehot(rel == lane + g * 128) for g in range(depth // 128)], axis=1)
        return jnp.dot(hot, xall[owner, first : first + depth, :], preferred_element_type=F32)

    def gather(owner, first, depth, fresh=False):
        n = 2 * cap

        def some(i, carry):
            rows = pl.ds(pl.multiple_of(i * n, n), n)
            got = picks(rows, owner, first, depth).astype(BF16)
            pk[rows, :] = got if fresh else pk[rows, :] + got
            return carry

        lax.fori_loop(0, n_exp * cap // n, some, 0)

    def from_sib(owner, cs):
        for c in cs:
            ag(owner, c, ags_sem.at[0], sib).wait_recv()

    xs, ys, ds = sib + dx, sib + dy, sib + dx + dy
    hb = tok // 2
    lo, hi = range(half), range(half, CHUNKS)

    def slot(i):
        nonlocal nx, ny, ns
        if i < CHUNKS:
            a, ca, b, cb = xn, i, yn, yorder[i]
        else:
            a, ca, b, cb = dg, i - CHUNKS, dg, yorder[i - CHUNKS]
        ag(a, ca, agx_sem.at[0], xn).wait_recv()
        ag(b, cb, agy_sem.at[0], yn).wait_recv()
        if i < half:
            go(ag(a, ca, agy_sem.at[ny], yn))
            go(ag(b, cb, agx_sem.at[nx], xn))
            nx, ny = nx + 1, ny + 1
        go(ag(a, ca, ags_sem.at[ns], sib))
        go(ag(b, cb, ags_sem.at[ns + 1], sib))
        ns += 2

    gather(me, 0, hb, True)
    slot(0)
    gather(me, hb, hb)
    slot(1)
    from_sib(sib, lo)
    gather(sib, 0, hb)
    slot(2)
    from_sib(sib, hi)
    gather(sib, hb, hb)
    slot(3)
    gather(xn, 0, hb)
    slot(4)
    gather(yn, hb, hb)
    slot(5)
    from_sib(xs, lo)
    gather(xs, 0, hb)
    slot(6)
    from_sib(ys, hi)
    gather(ys, hb, hb)
    slot(7)
    gather(xn, hb, hb)
    slot(8)
    gather(yn, 0, hb)
    from_sib(xs, hi)
    slot(9)
    gather(xs, hb, hb)
    slot(10)
    from_sib(ys, lo)
    gather(ys, 0, hb)
    qb = hb // 2
    gather(dg, 0, qb)
    gather(dg, tok - qb, qb)
    slot(11)
    from_sib(ds, (0, 1, CHUNKS - 2, CHUNKS - 1))
    gather(ds, 0, qb)
    gather(ds, tok - qb, qb)
    from_sib(ds, range(2, CHUNKS - 2))

    for k, dev in enumerate(peers):
        remote(rt_send.at[dev], rt_recv.at[dev], rts_sem.at[k], rtr_sem.at[dev], dev).wait_recv()
    for p in range(NDEV // 2):
        rowtab[:, p * 128 : (p + 1) * 128] = rt_recv[2 * p] + rt_recv[2 * p + 1] - 1.0
    yacc[...] = xall[me].astype(F32)

    def ret_copy(e, k, dev, src_dev):
        return remote(
            send.at[e, pl.ds(dev * slots, slots), :], ret.at[e, src_dev], snd_sem.at[e, k], rcv_sem.at[e, src_dev], dev
        )

    def loc_copy(e):
        return pltpu.make_async_copy(send.at[e, pl.ds(me * slots, slots), :], ret.at[e, me], loc_sem.at[e])

    def produce(e):
        rows = pl.ds(pl.multiple_of(e * cap, cap), cap)
        late = picks(rows, dg, qb, hb) + picks(rows, ds, qb, hb)
        pk[rows, :] = pk[rows, :] + late.astype(BF16)
        code = code_s[pl.ds(e, 1), :].astype(jnp.int32)
        pmat[...] = _onehot(jnp.broadcast_to(code, (nslot, cap)) == _iota((nslot, cap), 0))

        up_copy(e).wait()
        tile = 1024

        def up(j, carry):
            cols = pl.ds(pl.multiple_of(j * tile, tile), tile)
            z = jnp.dot(pk[rows, :], wup[e % 2, :, cols], preferred_element_type=F32)
            hid[:, cols] = _gelu(z).astype(BF16)
            return carry

        lax.fori_loop(0, ff // tile, up, 0)

        @pl.when(e + 2 < n_exp)
        def _():
            up_copy(e + 2).start()

        down_copy(e).wait()

        o = jnp.dot(hid[...], wdn[e % 2], preferred_element_type=F32)
        gate = jnp.concatenate([gate_b[rows, :]] * (width // 128), axis=1)
        contrib = (o * gate).astype(BF16)
        send[e] = jnp.dot(pmat[...], contrib, preferred_element_type=F32).astype(BF16)

        @pl.when(e + 2 < n_exp)
        def _():
            down_copy(e + 2).start()

        for k, dev in enumerate(peers):
            ret_copy(e, k, dev, me).start()
        loc_copy(e).start()

    def combine(e):
        loc_copy(e).wait()
        for k, dev in enumerate(peers):
            ret_copy(e, k, dev, dev).wait_recv()
        row = rowtab[pl.ds(e, 1), :].astype(jnp.int32)
        tile = 256

        def add(j, carry):
            rows = pl.ds(pl.multiple_of(j * tile, tile), tile)
            s = _onehot(jnp.broadcast_to(row, (tile, nslot)) == _iota((tile, nslot), 0) + j * tile)
            yacc[rows, :] += jnp.dot(s, ret[e].reshape(nslot, width), preferred_element_type=F32)
            return carry

        lax.fori_loop(0, tok // tile, add, 0)

    def step(e, carry):
        produce(e)

        @pl.when(e >= LAG)
        def _():
            combine(e - LAG)

        return carry

    lax.fori_loop(0, n_exp, step, 0)

    def rest(e, carry):
        combine(e)
        return carry

    lax.fori_loop(n_exp - LAG, n_exp, rest, 0)
    y_ref[...] = yacc[...].astype(BF16)

    for copy in sends:
        copy.wait_send()

    def drain(e, carry):
        for k, dev in enumerate(peers):
            ret_copy(e, k, dev, me).wait_send()
        return carry

    lax.fori_loop(0, n_exp, drain, 0)


def solution(mesh):
    def local_layer(x_loc, sel_loc, gate_loc, up_loc, down_loc):
        tok, width = x_loc.shape
        n_exp, cap = sel_loc.shape
        ff = up_loc.shape[2]
        slots = 2 * cap // NDEV
        nslot = NDEV * slots
        dma = pltpu.SemaphoreType.DMA
        vmem = pl.BlockSpec(memory_space=pltpu.VMEM)
        hbm = pl.BlockSpec(memory_space=pl.ANY)
        return pl.pallas_call(
            functools.partial(kernel, slots),
            out_shape=jax.ShapeDtypeStruct((tok, width), BF16),
            in_specs=[hbm, vmem, vmem, hbm, hbm],
            out_specs=vmem,
            scratch_shapes=[
                pltpu.VMEM((NDEV, tok, width), BF16),
                pltpu.VMEM((2, width, ff), BF16),
                pltpu.VMEM((2, ff, width), BF16),
                pltpu.VMEM((n_exp, nslot, width), BF16),
                pltpu.VMEM((n_exp, NDEV, slots, width), BF16),
                pltpu.VMEM((n_exp * cap, width), BF16),
                pltpu.VMEM((cap, ff), BF16),
                pltpu.VMEM((nslot, cap), BF16),
                pltpu.VMEM((tok, width), F32),
                pltpu.VMEM((n_exp * cap, 128), jnp.int32),
                pltpu.VMEM((n_exp * cap, 128), F32),
                pltpu.VMEM((n_exp, cap), F32),
                pltpu.VMEM((NDEV, n_exp, 128), F32),
                pltpu.VMEM((NDEV, n_exp, 128), F32),
                pltpu.VMEM((n_exp, nslot), F32),
                dma,
                dma((2,)),
                dma((2,)),
                dma((CHUNKS + CHUNKS // 2,)),
                dma((CHUNKS + CHUNKS // 2,)),
                dma((4 * CHUNKS,)),
                dma((NDEV, CHUNKS)),
                dma((NDEV - 1,)),
                dma((NDEV,)),
                dma((n_exp, NDEV - 1)),
                dma((n_exp, NDEV)),
                dma((n_exp,)),
            ],
            compiler_params=pltpu.CompilerParams(
                collective_id=0, has_side_effects=True, vmem_limit_bytes=67_000_000
            ),
            name="moe",
        )(x_loc, sel_loc, gate_loc, up_loc, down_loc)

    row_spec = P(("dp", "ep"), None)
    weight_spec = P("ep", None, None)
    return jax.shard_map(
        local_layer,
        mesh=mesh,
        in_specs=(row_spec, row_spec, row_spec, weight_spec, weight_spec),
        out_specs=row_spec,
        check_vma=False,
    )
```

```python
import functools

import jax
import jax.numpy as jnp
from jax import lax
from jax.experimental import pallas as pl
from jax.experimental.pallas import tpu as pltpu
from jax.sharding import PartitionSpec as P

F32 = jnp.float32
BF16 = jnp.bfloat16
MESH = pl.DeviceIdType.MESH

NDEV = 8
CHUNKS = 8


def _gelu(z):
    return 0.5 * z * (1.0 + jnp.tanh(0.7978845608028654 * (z + 0.044715 * (z * z * z))))


def _iota(shape, dim):
    return lax.broadcasted_iota(jnp.int32, shape, dim)


def _onehot(cond):
    return jnp.where(cond, 1.0, 0.0).astype(BF16)


def kernel(
    slots,
    x_ref, sel_ref, gate_ref, up_ref, down_ref,
    y_ref,
    xall, wup, wdn, send, ret, pk, hid, dpk, yacc,
    sel_b, gate_b, code_s, rt_send, rt_recv, rowtab,
    own_sem, wup_sem, wdn_sem, agx_sem, agy_sem, ags_sem, agr_sem,
    rts_sem, rtr_sem, snd_sem, rcv_sem, loc_sem, out_sem,
):
    n_exp, cap = sel_ref.shape
    tok, width = x_ref.shape
    ff = up_ref.shape[2]
    nslot = NDEV * slots
    me = lax.axis_index("ep")
    core = me % 2
    sib = me + 1 - 2 * core
    xx = (me // 2) % 2
    yy = me // 4
    dx = 2 - 4 * xx
    dy = 4 - 8 * yy
    xn, yn, dg = me + dx, me + dy, me + dx + dy
    peers = (dg, sib + dx + dy, xn, sib + dx, yn, sib + dy, sib)
    ch = tok // CHUNKS
    half = CHUNKS // 2
    yorder = [*range(CHUNKS - 1, half - 1, -1), *range(half)]

    def remote(src, dst, ssem, rsem, dev):
        return pltpu.make_async_remote_copy(
            src_ref=src, dst_ref=dst, send_sem=ssem, recv_sem=rsem, device_id={"ep": dev}, device_id_type=MESH
        )

    def up_copy(e):
        return pltpu.make_async_copy(up_ref.at[e], wup.at[e % 2], wup_sem.at[e % 2])

    def down_copy(e):
        return pltpu.make_async_copy(down_ref.at[e], wdn.at[e % 2], wdn_sem.at[e % 2])

    own_copy = pltpu.make_async_copy(x_ref, xall.at[me], own_sem)
    own_copy.start()

    barrier = pltpu.get_barrier_semaphore()
    for dev in (sib, xn, yn):
        pl.semaphore_signal(barrier, inc=1, device_id={"ep": dev}, device_id_type=MESH)
    pl.semaphore_wait(barrier, 3)
    own_copy.wait()

    def piece(owner, c):
        return xall.at[owner, pl.ds(c * ch, ch), :]

    def ag(owner, c, ssem, dev):
        return remote(piece(owner, c), piece(owner, c), ssem, agr_sem.at[owner, c], dev)

    sends = []

    def go(copy):
        copy.start()
        sends.append(copy)

    nx, ny, ns = 0, 0, 0
    for i in range(CHUNKS):
        go(ag(me, i, agx_sem.at[nx], xn))
        go(ag(me, yorder[i], agy_sem.at[ny], yn))
        go(ag(me, i, ags_sem.at[ns], sib))
        nx, ny, ns = nx + 1, ny + 1, ns + 1

    for e in range(2):
        up_copy(e).start()
        down_copy(e).start()

    sel_cols = jnp.transpose(sel_ref[...].astype(F32)).astype(jnp.int32)
    gate_cols = jnp.transpose(gate_ref[...])
    for e in range(n_exp):
        sel_b[e * cap : (e + 1) * cap, :] = jnp.broadcast_to(sel_cols[:, e : e + 1], (cap, 128))
        gate_b[e * cap : (e + 1) * cap, :] = jnp.broadcast_to(gate_cols[:, e : e + 1], (cap, 128))
    upper = _onehot(_iota((cap, cap), 0) < _iota((cap, cap), 1))
    for e in range(n_exp):
        sel_row = sel_ref[pl.ds(e, 1), :]
        owner = lax.shift_right_logical(sel_row, 10)
        local = jnp.bitwise_and(sel_row, 1023)
        mine = jnp.broadcast_to(owner, (16, cap)) == _iota((16, cap), 0)
        cum = jnp.dot(_onehot(mine), upper, preferred_element_type=F32)
        rank = jnp.sum(jnp.where(mine, cum, 0.0), axis=0, keepdims=True)
        owner_f = owner.astype(F32)
        code_s[pl.ds(e, 1), :] = owner_f * slots + rank
        tcode = (owner_f * 128 + rank).astype(jnp.int32) + core * slots
        q = _onehot(jnp.broadcast_to(tcode, (NDEV * 128, cap)) == _iota((NDEV * 128, cap), 0))
        hi = lax.shift_right_logical(local, 5).astype(F32)
        lo = jnp.bitwise_and(local, 31).astype(F32)
        rows = _iota((16, cap), 0)
        lhs = jnp.where(rows == 0, hi, jnp.where(rows == 1, lo, jnp.where(rows == 2, 1.0, 0.0))).astype(BF16)
        t = lax.dot_general(lhs, q, (((1,), (1,)), ((), ())), preferred_element_type=F32)
        tab = t[0:1] * 32.0 + t[1:2] + t[2:3]
        for g in range(NDEV):
            rt_send[g, pl.ds(e, 1), :] = tab[:, g * 128 : (g + 1) * 128]
    rt_recv[me] = rt_send[me]
    yacc[...] = xall[me].astype(F32)
    def picks(rows, owner, first, depth):
        n = rows.size
        rel = sel_b[rows, :] - (owner * tok + first)
        lane = _iota((n, 128), 1)
        hot = jnp.concatenate([_onehot(rel == lane + g * 128) for g in range(depth // 128)], axis=1)
        return jnp.dot(hot, xall[owner, first : first + depth, :], preferred_element_type=F32)

    def gather(owner, first, depth, pairs=(0, n_exp // 2), fresh=False):
        n = 2 * cap

        def some(i, carry):
            rows = pl.ds(pl.multiple_of(i * n, n), n)
            got = picks(rows, owner, first, depth).astype(BF16)
            pk[rows, :] = got if fresh else pk[rows, :] + got
            return carry

        lax.fori_loop(*pairs, some, 0)

    def from_sib(owner, cs):
        for c in cs:
            ag(owner, c, ags_sem.at[0], sib).wait_recv()

    xs, ys, ds = sib + dx, sib + dy, sib + dx + dy
    hb = tok // 2
    lo, hi = range(half), range(half, CHUNKS)

    def slot(i):
        nonlocal nx, ny, ns
        if i < CHUNKS:
            a, ca, b, cb = xn, i, yn, yorder[i]
        else:
            a, ca, b, cb = dg, i - CHUNKS, dg, yorder[i - CHUNKS]
        ag(a, ca, agx_sem.at[0], xn).wait_recv()
        ag(b, cb, agy_sem.at[0], yn).wait_recv()
        if i < half:
            go(ag(a, ca, agy_sem.at[ny], yn))
            go(ag(b, cb, agx_sem.at[nx], xn))
            nx, ny = nx + 1, ny + 1
        go(ag(a, ca, ags_sem.at[ns], sib))
        go(ag(b, cb, ags_sem.at[ns + 1], sib))
        ns += 2

    def ret_copy(e, k, src_dev):
        dev = peers[k]
        return remote(
            send.at[e, pl.ds(dev * slots, slots), :], ret.at[e, src_dev], snd_sem.at[e, k], rcv_sem.at[e, src_dev], dev
        )

    def loc_copy(e):
        return pltpu.make_async_copy(send.at[e, pl.ds(me * slots, slots), :], ret.at[e, me], loc_sem.at[e])

    def up(lhs, m, e):
        up_copy(e).wait()
        tile = 1024

        def some(j, carry):
            cols = pl.ds(pl.multiple_of(j * tile, tile), tile)
            z = jnp.dot(lhs[...], wup[e % 2, :, cols], preferred_element_type=F32)
            hid[0:m, cols] = _gelu(z).astype(BF16)
            return carry

        lax.fori_loop(0, ff // tile, some, 0)

    def scatter(e, rows):
        code = code_s[pl.ds(e, 1), :].astype(jnp.int32)
        place = _onehot(jnp.broadcast_to(code, (nslot, cap)) == _iota((nslot, cap), 0))
        o = jnp.dot(hid[...], wdn[e % 2], preferred_element_type=F32)
        gate = jnp.concatenate([gate_b[rows, :]] * (width // 128), axis=1)
        contrib = (o * gate).astype(BF16)
        send[e] = jnp.dot(place, contrib, preferred_element_type=F32).astype(BF16)

    def early(e):
        rows = pl.ds(e * cap, cap)
        up(pk.at[rows, :], cap, e)
        down_copy(e).wait()
        scatter(e, rows)
        for k in range(2, NDEV - 1):
            ret_copy(e, k, me).start()
        loc_copy(e).start()

    def diagonal(e, carry):
        rows = pl.ds(pl.multiple_of(e * cap, cap), cap)
        m = 2 * slots
        base = pl.multiple_of((dg // 2) * m, m)
        code = code_s[pl.ds(e, 1), :].astype(jnp.int32) - base
        here = jnp.broadcast_to(code, (m, cap)) == _iota((m, cap), 0)
        gate = jnp.sum(jnp.where(here, gate_ref[pl.ds(e, 1), :], 0.0), axis=1, keepdims=True)
        dpk[...] = jnp.dot(_onehot(here), pk[rows, :], preferred_element_type=F32).astype(BF16)
        tile = 1024

        def some(j, c):
            cols = pl.ds(pl.multiple_of(j * tile, tile), tile)
            z = jnp.dot(dpk[...], wup[e % 2, :, cols], preferred_element_type=F32)
            hid[0:m, cols] = _gelu(z).astype(BF16)
            return c

        lax.fori_loop(0, ff // tile, some, 0)
        up_copy(e + 2).start()
        o = jnp.dot(hid[0:m, :], wdn[e % 2], preferred_element_type=F32)
        send[e, pl.ds(base, m), :] = (o * gate).astype(BF16)
        down_copy(e + 2).start()
        for k in range(2):
            ret_copy(e, k, me).start()
        return carry

    def produce(e):
        rows = pl.ds(pl.multiple_of(e * cap, cap), cap)
        up(pk.at[rows, :], cap, e)

        @pl.when(e + 2 < n_exp)
        def _():
            up_copy(e + 2).start()

        down_copy(e).wait()
        scatter(e, rows)

        @pl.when(e + 2 < n_exp)
        def _():
            down_copy(e + 2).start()

        for k in range(NDEV - 1):
            ret_copy(e, k, me).start()
        loc_copy(e).start()

    def arrived(e):
        loc_copy(e).wait()
        for k, dev in enumerate(peers):
            ret_copy(e, k, dev).wait_recv()

    def adds(e, j, tile):
        row = rowtab[pl.ds(e, 1), :].astype(jnp.int32)
        hot = _onehot(jnp.broadcast_to(row, (tile, nslot)) == _iota((tile, nslot), 0) + j * tile)
        return jnp.dot(hot, ret[e].reshape(nslot, width), preferred_element_type=F32)

    def combine(e):
        arrived(e)
        tile = 256

        def some(j, carry):
            rows = pl.ds(pl.multiple_of(j * tile, tile), tile)
            yacc[rows, :] += adds(e, j, tile)
            return carry

        lax.fori_loop(0, tok // tile, some, 0)

    qb = hb // 2
    gather(me, 0, hb, fresh=True)
    slot(0)
    gather(me, hb, hb)
    slot(1)
    from_sib(sib, lo)
    gather(sib, 0, hb)
    slot(2)
    from_sib(sib, hi)
    gather(sib, hb, hb)
    slot(3)
    gather(xn, 0, hb)
    from_sib(xs, lo)
    slot(4)
    for k, dev in enumerate(peers):
        go(remote(rt_send.at[dev], rt_recv.at[me], rts_sem.at[k], rtr_sem.at[me], dev))
    gather(yn, hb, hb)
    gather(xs, 0, hb)
    slot(5)
    from_sib(ys, hi)
    gather(ys, hb, hb)
    gather(xn, hb, qb)
    slot(6)
    gather(yn, 0, qb)
    from_sib(xs, (4, 5))
    gather(xs, hb, qb)
    from_sib(ys, (0, 1))
    gather(ys, 0, qb)
    slot(7)
    first, later = (0, 1), (1, n_exp // 2)

    def third(pairs):
        gather(xn, hb + qb, qb, pairs)
        gather(yn, qb, qb, pairs)
        gather(xs, hb + qb, qb, pairs)
        gather(ys, qb, qb, pairs)

    from_sib(xs, (6, 7))
    from_sib(ys, (2, 3))
    third(first)
    early(0)
    slot(8)
    early(1)
    slot(9)
    third(later)
    slot(10)
    from_sib(ds, (0, 1, CHUNKS - 2, CHUNKS - 1))
    for dev in (dg, ds):
        gather(dev, 0, qb, first)
        gather(dev, tok - qb, qb, first)
    slot(11)
    from_sib(ds, range(2, CHUNKS - 2))
    for dev in (dg, ds):
        gather(dev, qb, hb, first)

    lax.fori_loop(0, 2, diagonal, 0)

    for k, dev in enumerate(peers):
        remote(rt_send.at[dev], rt_recv.at[dev], rts_sem.at[k], rtr_sem.at[dev], dev).wait_recv()
    for p in range(NDEV // 2):
        rowtab[:, p * 128 : (p + 1) * 128] = rt_recv[2 * p] + rt_recv[2 * p + 1] - 1.0

    def pair(p, carry):
        for dev in (dg, ds):
            gather(dev, 0, tok, (p, p + 1))
        produce(2 * p)

        @pl.when(p >= 2)
        def _():
            combine(2 * p - 3)

        produce(2 * p + 1)
        combine(2 * p - 2)
        return carry

    lax.fori_loop(1, n_exp // 2, pair, 0)

    def rest(e, carry):
        combine(e)
        return carry

    lax.fori_loop(n_exp - 3, n_exp - 1, rest, 0)
    last = n_exp - 1
    arrived(last)
    tile = 256
    outs = []
    for j in range(tok // tile):
        rows = pl.ds(j * tile, tile)
        pk[rows, :] = (yacc[rows, :] + adds(last, j, tile)).astype(BF16)
        outs.append(pltpu.make_async_copy(pk.at[rows, :], y_ref.at[rows, :], out_sem.at[j]))
        outs[-1].start()

    for copy in sends:
        copy.wait_send()

    def drain(e, carry):
        for k in range(NDEV - 1):
            ret_copy(e, k, me).wait_send()
        return carry

    lax.fori_loop(0, n_exp, drain, 0)
    for copy in outs:
        copy.wait()


def solution(mesh):
    def local_layer(x_loc, sel_loc, gate_loc, up_loc, down_loc):
        tok, width = x_loc.shape
        n_exp, cap = sel_loc.shape
        ff = up_loc.shape[2]
        slots = 2 * cap // NDEV
        nslot = NDEV * slots
        dma = pltpu.SemaphoreType.DMA
        vmem = pl.BlockSpec(memory_space=pltpu.VMEM)
        hbm = pl.BlockSpec(memory_space=pl.ANY)
        return pl.pallas_call(
            functools.partial(kernel, slots),
            out_shape=jax.ShapeDtypeStruct((tok, width), BF16),
            in_specs=[hbm, vmem, vmem, hbm, hbm],
            out_specs=hbm,
            scratch_shapes=[
                pltpu.VMEM((NDEV, tok, width), BF16),
                pltpu.VMEM((2, width, ff), BF16),
                pltpu.VMEM((2, ff, width), BF16),
                pltpu.VMEM((n_exp, nslot, width), BF16),
                pltpu.VMEM((n_exp, NDEV, slots, width), BF16),
                pltpu.VMEM((n_exp * cap, width), BF16),
                pltpu.VMEM((cap, ff), BF16),
                pltpu.VMEM((2 * slots, width), BF16),
                pltpu.VMEM((tok, width), F32),
                pltpu.VMEM((n_exp * cap, 128), jnp.int32),
                pltpu.VMEM((n_exp * cap, 128), F32),
                pltpu.VMEM((n_exp, cap), F32),
                pltpu.VMEM((NDEV, n_exp, 128), F32),
                pltpu.VMEM((NDEV, n_exp, 128), F32),
                pltpu.VMEM((n_exp, nslot), F32),
                dma,
                dma((2,)),
                dma((2,)),
                dma((CHUNKS + CHUNKS // 2,)),
                dma((CHUNKS + CHUNKS // 2,)),
                dma((4 * CHUNKS,)),
                dma((NDEV, CHUNKS)),
                dma((NDEV - 1,)),
                dma((NDEV,)),
                dma((n_exp, NDEV - 1)),
                dma((n_exp, NDEV)),
                dma((n_exp,)),
                dma((4,)),
            ],
            compiler_params=pltpu.CompilerParams(
                collective_id=0, has_side_effects=True, vmem_limit_bytes=67_000_000
            ),
            name="moe",
        )(x_loc, sel_loc, gate_loc, up_loc, down_loc)

    row_spec = P(("dp", "ep"), None)
    weight_spec = P("ep", None, None)
    return jax.shard_map(
        local_layer,
        mesh=mesh,
        in_specs=(row_spec, row_spec, row_spec, weight_spec, weight_spec),
        out_specs=row_spec,
        check_vma=False,
    )
```

```python
import functools

import jax
import jax.numpy as jnp
from jax import lax
from jax.experimental import pallas as pl
from jax.experimental.pallas import tpu as pltpu
from jax.sharding import PartitionSpec as P

F32 = jnp.float32
BF16 = jnp.bfloat16
MESH = pl.DeviceIdType.MESH

NDEV = 8
CHUNKS = 8


def _gelu(z):
    return 0.5 * z * (1.0 + jnp.tanh(0.7978845608028654 * (z + 0.044715 * (z * z * z))))


def _iota(shape, dim):
    return lax.broadcasted_iota(jnp.int32, shape, dim)


def _onehot(cond):
    return jnp.where(cond, 1.0, 0.0).astype(BF16)


def kernel(
    slots,
    x_ref, sel_hbm, gate_hbm, up_ref, down_ref,
    y_ref,
    sel_ref, gate_ref, xall, wup, wdn, send, ret, pk, hid, dpk, yacc,
    sel_b, gate_b, code_s, rt_send, rt_recv, rowtab,
    own_sem, wup_sem, wdn_sem, agx_sem, agy_sem, ags_sem, agr_sem,
    rts_sem, rtr_sem, snd_sem, rcv_sem, loc_sem, in_sem,
):
    n_exp, cap = sel_ref.shape
    tok, width = x_ref.shape
    ff = up_ref.shape[2]
    nslot = NDEV * slots
    me = lax.axis_index("ep")
    core = me % 2
    sib = me + 1 - 2 * core
    xx = (me // 2) % 2
    yy = me // 4
    dx = 2 - 4 * xx
    dy = 4 - 8 * yy
    xn, yn, dg = me + dx, me + dy, me + dx + dy
    peers = (dg, sib + dx + dy, xn, sib + dx, yn, sib + dy, sib)
    ch = tok // CHUNKS
    half = CHUNKS // 2
    yorder = [*range(CHUNKS - 1, half - 1, -1), *range(half)]

    def remote(src, dst, ssem, rsem, dev):
        return pltpu.make_async_remote_copy(
            src_ref=src, dst_ref=dst, send_sem=ssem, recv_sem=rsem, device_id={"ep": dev}, device_id_type=MESH
        )

    def up_copy(e):
        return pltpu.make_async_copy(up_ref.at[e], wup.at[e % 2], wup_sem.at[e % 2])

    def down_copy(e):
        return pltpu.make_async_copy(down_ref.at[e], wdn.at[e % 2], wdn_sem.at[e % 2])

    own_copy = pltpu.make_async_copy(x_ref, xall.at[me], own_sem)
    own_copy.start()
    sel_copy = pltpu.make_async_copy(sel_hbm, sel_ref, in_sem.at[0])
    gate_copy = pltpu.make_async_copy(gate_hbm, gate_ref, in_sem.at[1])
    sel_copy.start()
    gate_copy.start()

    barrier = pltpu.get_barrier_semaphore()
    for dev in (sib, xn, yn):
        pl.semaphore_signal(barrier, inc=1, device_id={"ep": dev}, device_id_type=MESH)
    pl.semaphore_wait(barrier, 3)
    own_copy.wait()

    def piece(owner, c):
        return xall.at[owner, pl.ds(c * ch, ch), :]

    def ag(owner, c, ssem, dev):
        return remote(piece(owner, c), piece(owner, c), ssem, agr_sem.at[owner, c], dev)

    sends = []

    def go(copy):
        copy.start()
        sends.append(copy)

    nx, ny, ns = 0, 0, 0
    for i in range(CHUNKS):
        go(ag(me, i, agx_sem.at[nx], xn))
        go(ag(me, yorder[i], agy_sem.at[ny], yn))
        go(ag(me, i, ags_sem.at[ns], sib))
        nx, ny, ns = nx + 1, ny + 1, ns + 1

    for e in range(2):
        up_copy(e).start()
        down_copy(e).start()

    sel_copy.wait()
    gate_copy.wait()

    sel_cols = jnp.transpose(sel_ref[...].astype(F32)).astype(jnp.int32)
    gate_cols = jnp.transpose(gate_ref[...])
    for e in range(n_exp):
        sel_b[e * cap : (e + 1) * cap, :] = jnp.broadcast_to(sel_cols[:, e : e + 1], (cap, 128))
        gate_b[e * cap : (e + 1) * cap, :] = jnp.broadcast_to(gate_cols[:, e : e + 1], (cap, 128))
    upper = _onehot(_iota((cap, cap), 0) < _iota((cap, cap), 1))
    for e in range(n_exp):
        sel_row = sel_ref[pl.ds(e, 1), :]
        owner = lax.shift_right_logical(sel_row, 10)
        local = jnp.bitwise_and(sel_row, 1023)
        mine = jnp.broadcast_to(owner, (16, cap)) == _iota((16, cap), 0)
        cum = jnp.dot(_onehot(mine), upper, preferred_element_type=F32)
        rank = jnp.sum(jnp.where(mine, cum, 0.0), axis=0, keepdims=True)
        owner_f = owner.astype(F32)
        code_s[pl.ds(e, 1), :] = owner_f * slots + rank
        tcode = (owner_f * 128 + rank).astype(jnp.int32) + core * slots
        q = _onehot(jnp.broadcast_to(tcode, (NDEV * 128, cap)) == _iota((NDEV * 128, cap), 0))
        hi = lax.shift_right_logical(local, 5).astype(F32)
        lo = jnp.bitwise_and(local, 31).astype(F32)
        rows = _iota((16, cap), 0)
        lhs = jnp.where(rows == 0, hi, jnp.where(rows == 1, lo, jnp.where(rows == 2, 1.0, 0.0))).astype(BF16)
        t = lax.dot_general(lhs, q, (((1,), (1,)), ((), ())), preferred_element_type=F32)
        tab = t[0:1] * 32.0 + t[1:2] + t[2:3]
        for g in range(NDEV):
            rt_send[g, pl.ds(e, 1), :] = tab[:, g * 128 : (g + 1) * 128]
    rt_recv[me] = rt_send[me]
    yacc[...] = xall[me].astype(F32)
    def picks(rows, owner, first, depth):
        n = rows.size
        rel = sel_b[rows, :] - (owner * tok + first)
        lane = _iota((n, 128), 1)
        hot = jnp.concatenate([_onehot(rel == lane + g * 128) for g in range(depth // 128)], axis=1)
        return jnp.dot(hot, xall[owner, first : first + depth, :], preferred_element_type=F32)

    def gather(owner, first, depth, pairs=(0, n_exp // 2), fresh=False):
        n = 2 * cap

        def some(i, carry):
            rows = pl.ds(pl.multiple_of(i * n, n), n)
            got = picks(rows, owner, first, depth).astype(BF16)
            pk[rows, :] = got if fresh else pk[rows, :] + got
            return carry

        lax.fori_loop(*pairs, some, 0)

    def from_sib(owner, cs):
        for c in cs:
            ag(owner, c, ags_sem.at[0], sib).wait_recv()

    xs, ys, ds = sib + dx, sib + dy, sib + dx + dy
    hb = tok // 2
    lo, hi = range(half), range(half, CHUNKS)

    def slot(i):
        nonlocal nx, ny, ns
        if i < CHUNKS:
            a, ca, b, cb = xn, i, yn, yorder[i]
        else:
            a, ca, b, cb = dg, i - CHUNKS, dg, yorder[i - CHUNKS]
        ag(a, ca, agx_sem.at[0], xn).wait_recv()
        ag(b, cb, agy_sem.at[0], yn).wait_recv()
        if i < half:
            go(ag(a, ca, agy_sem.at[ny], yn))
            go(ag(b, cb, agx_sem.at[nx], xn))
            nx, ny = nx + 1, ny + 1
        go(ag(a, ca, ags_sem.at[ns], sib))
        go(ag(b, cb, ags_sem.at[ns + 1], sib))
        ns += 2

    def ret_copy(e, k, src_dev):
        dev = peers[k]
        return remote(
            send.at[e, pl.ds(dev * slots, slots), :], ret.at[e, src_dev], snd_sem.at[e, k], rcv_sem.at[e, src_dev], dev
        )

    def loc_copy(e):
        return pltpu.make_async_copy(send.at[e, pl.ds(me * slots, slots), :], ret.at[e, me], loc_sem.at[e])

    def up(lhs, m, e):
        up_copy(e).wait()
        tile = 1024

        def some(j, carry):
            cols = pl.ds(pl.multiple_of(j * tile, tile), tile)
            z = jnp.dot(lhs[...], wup[e % 2, :, cols], preferred_element_type=F32)
            hid[0:m, cols] = _gelu(z).astype(BF16)
            return carry

        lax.fori_loop(0, ff // tile, some, 0)

    def scatter(e, rows):
        code = code_s[pl.ds(e, 1), :].astype(jnp.int32)
        place = _onehot(jnp.broadcast_to(code, (nslot, cap)) == _iota((nslot, cap), 0))
        o = jnp.dot(hid[...], wdn[e % 2], preferred_element_type=F32)
        gate = jnp.concatenate([gate_b[rows, :]] * (width // 128), axis=1)
        contrib = (o * gate).astype(BF16)
        send[e] = jnp.dot(place, contrib, preferred_element_type=F32).astype(BF16)

    def early(e):
        rows = pl.ds(e * cap, cap)
        up(pk.at[rows, :], cap, e)
        down_copy(e).wait()
        scatter(e, rows)
        for k in range(2, NDEV - 1):
            ret_copy(e, k, me).start()
        loc_copy(e).start()

    def diagonal(e, carry):
        rows = pl.ds(pl.multiple_of(e * cap, cap), cap)
        m = 2 * slots
        base = pl.multiple_of((dg // 2) * m, m)
        code = code_s[pl.ds(e, 1), :].astype(jnp.int32) - base
        here = jnp.broadcast_to(code, (m, cap)) == _iota((m, cap), 0)
        gate = jnp.sum(jnp.where(here, gate_ref[pl.ds(e, 1), :], 0.0), axis=1, keepdims=True)
        dpk[...] = jnp.dot(_onehot(here), pk[rows, :], preferred_element_type=F32).astype(BF16)
        tile = 1024

        def some(j, c):
            cols = pl.ds(pl.multiple_of(j * tile, tile), tile)
            z = jnp.dot(dpk[...], wup[e % 2, :, cols], preferred_element_type=F32)
            hid[0:m, cols] = _gelu(z).astype(BF16)
            return c

        lax.fori_loop(0, ff // tile, some, 0)
        up_copy(e + 2).start()
        o = jnp.dot(hid[0:m, :], wdn[e % 2], preferred_element_type=F32)
        send[e, pl.ds(base, m), :] = (o * gate).astype(BF16)
        down_copy(e + 2).start()
        for k in range(2):
            ret_copy(e, k, me).start()
        return carry

    def produce(e):
        rows = pl.ds(pl.multiple_of(e * cap, cap), cap)
        up(pk.at[rows, :], cap, e)

        @pl.when(e + 2 < n_exp)
        def _():
            up_copy(e + 2).start()

        down_copy(e).wait()
        scatter(e, rows)

        @pl.when(e + 2 < n_exp)
        def _():
            down_copy(e + 2).start()

        for k in range(NDEV - 1):
            ret_copy(e, k, me).start()
        loc_copy(e).start()

    def arrived(e):
        loc_copy(e).wait()
        for k, dev in enumerate(peers):
            ret_copy(e, k, dev).wait_recv()

    def adds(e, j, tile):
        row = rowtab[pl.ds(e, 1), :].astype(jnp.int32)
        hot = _onehot(jnp.broadcast_to(row, (tile, nslot)) == _iota((tile, nslot), 0) + j * tile)
        return jnp.dot(hot, ret[e].reshape(nslot, width), preferred_element_type=F32)

    def combine(e):
        arrived(e)
        tile = 256

        def some(j, carry):
            rows = pl.ds(pl.multiple_of(j * tile, tile), tile)
            yacc[rows, :] += adds(e, j, tile)
            return carry

        lax.fori_loop(0, tok // tile, some, 0)

    qb = hb // 2
    gather(me, 0, hb, fresh=True)
    slot(0)
    gather(me, hb, hb)
    slot(1)
    from_sib(sib, lo)
    gather(sib, 0, hb)
    slot(2)
    from_sib(sib, hi)
    gather(sib, hb, hb)
    slot(3)
    gather(xn, 0, hb)
    from_sib(xs, lo)
    slot(4)
    for k, dev in enumerate(peers):
        go(remote(rt_send.at[dev], rt_recv.at[me], rts_sem.at[k], rtr_sem.at[me], dev))
    gather(yn, hb, hb)
    gather(xs, 0, hb)
    slot(5)
    from_sib(ys, hi)
    gather(ys, hb, hb)
    gather(xn, hb, qb)
    slot(6)
    gather(yn, 0, qb)
    from_sib(xs, (4, 5))
    gather(xs, hb, qb)
    from_sib(ys, (0, 1))
    gather(ys, 0, qb)
    slot(7)
    first, later = (0, 1), (1, n_exp // 2)

    def third(pairs):
        gather(xn, hb + qb, qb, pairs)
        gather(yn, qb, qb, pairs)
        gather(xs, hb + qb, qb, pairs)
        gather(ys, qb, qb, pairs)

    from_sib(xs, (6, 7))
    from_sib(ys, (2, 3))
    third(first)
    early(0)
    slot(8)
    early(1)
    slot(9)
    third(later)
    slot(10)
    from_sib(ds, (0, 1, CHUNKS - 2, CHUNKS - 1))
    for dev in (dg, ds):
        gather(dev, 0, qb, first)
        gather(dev, tok - qb, qb, first)
    slot(11)
    from_sib(ds, range(2, CHUNKS - 2))
    for dev in (dg, ds):
        gather(dev, qb, hb, first)

    lax.fori_loop(0, 2, diagonal, 0)

    for k, dev in enumerate(peers):
        remote(rt_send.at[dev], rt_recv.at[dev], rts_sem.at[k], rtr_sem.at[dev], dev).wait_recv()
    for p in range(NDEV // 2):
        rowtab[:, p * 128 : (p + 1) * 128] = rt_recv[2 * p] + rt_recv[2 * p + 1] - 1.0

    def pair(p, carry):
        for dev in (dg, ds):
            gather(dev, 0, tok, (p, p + 1))
        produce(2 * p)

        @pl.when(p >= 2)
        def _():
            combine(2 * p - 3)

        produce(2 * p + 1)
        combine(2 * p - 2)
        return carry

    lax.fori_loop(1, n_exp // 2, pair, 0)

    def rest(e, carry):
        combine(e)
        return carry

    lax.fori_loop(n_exp - 3, n_exp - 1, rest, 0)
    last = n_exp - 1
    arrived(last)
    tile = 256

    def finish(j, carry):
        rows = pl.ds(pl.multiple_of(j * tile, tile), tile)
        y_ref[rows, :] = (yacc[rows, :] + adds(last, j, tile)).astype(BF16)
        return carry

    lax.fori_loop(0, tok // tile, finish, 0)

    for copy in sends:
        copy.wait_send()

    def drain(e, carry):
        for k in range(NDEV - 1):
            ret_copy(e, k, me).wait_send()
        return carry

    lax.fori_loop(0, n_exp, drain, 0)


def solution(mesh):
    def local_layer(x_loc, sel_loc, gate_loc, up_loc, down_loc):
        tok, width = x_loc.shape
        n_exp, cap = sel_loc.shape
        ff = up_loc.shape[2]
        slots = 2 * cap // NDEV
        nslot = NDEV * slots
        dma = pltpu.SemaphoreType.DMA
        vmem = pl.BlockSpec(memory_space=pltpu.VMEM)
        hbm = pl.BlockSpec(memory_space=pl.ANY)
        return pl.pallas_call(
            functools.partial(kernel, slots),
            out_shape=pltpu.VMEM((tok, width), BF16),
            in_specs=[hbm] * 5,
            out_specs=vmem,
            scratch_shapes=[
                pltpu.VMEM((n_exp, cap), jnp.int32),
                pltpu.VMEM((n_exp, cap), F32),
                pltpu.VMEM((NDEV, tok, width), BF16),
                pltpu.VMEM((2, width, ff), BF16),
                pltpu.VMEM((2, ff, width), BF16),
                pltpu.VMEM((n_exp, nslot, width), BF16),
                pltpu.VMEM((n_exp, NDEV, slots, width), BF16),
                pltpu.VMEM((n_exp * cap, width), BF16),
                pltpu.VMEM((cap, ff), BF16),
                pltpu.VMEM((2 * slots, width), BF16),
                pltpu.VMEM((tok, width), F32),
                pltpu.VMEM((n_exp * cap, 128), jnp.int32),
                pltpu.VMEM((n_exp * cap, 128), F32),
                pltpu.VMEM((n_exp, cap), F32),
                pltpu.VMEM((NDEV, n_exp, 128), F32),
                pltpu.VMEM((NDEV, n_exp, 128), F32),
                pltpu.VMEM((n_exp, nslot), F32),
                dma,
                dma((2,)),
                dma((2,)),
                dma((CHUNKS + CHUNKS // 2,)),
                dma((CHUNKS + CHUNKS // 2,)),
                dma((4 * CHUNKS,)),
                dma((NDEV, CHUNKS)),
                dma((NDEV - 1,)),
                dma((NDEV,)),
                dma((n_exp, NDEV - 1)),
                dma((n_exp, NDEV)),
                dma((n_exp,)),
                dma((2,)),
            ],
            compiler_params=pltpu.CompilerParams(
                collective_id=0, has_side_effects=True, vmem_limit_bytes=64_000_000
            ),
            name="moe",
        )(x_loc, sel_loc, gate_loc, up_loc, down_loc)

    row_spec = P(("dp", "ep"), None)
    weight_spec = P("ep", None, None)
    return jax.shard_map(
        local_layer,
        mesh=mesh,
        in_specs=(row_spec, row_spec, row_spec, weight_spec, weight_spec),
        out_specs=row_spec,
        check_vma=False,
    )
```

```python
import functools

import jax
import jax.numpy as jnp
from jax import lax
from jax.experimental import pallas as pl
from jax.experimental.pallas import tpu as pltpu
from jax.sharding import PartitionSpec as P

F32 = jnp.float32
BF16 = jnp.bfloat16
MESH = pl.DeviceIdType.MESH

NDEV = 8
CHUNKS = 8


def _gelu(z):
    return 0.5 * z * (1.0 + jnp.tanh(0.7978845608028654 * (z + 0.044715 * (z * z * z))))


def _iota(shape, dim):
    return lax.broadcasted_iota(jnp.int32, shape, dim)


def _onehot(cond):
    return jnp.where(cond, 1.0, 0.0).astype(BF16)


def kernel(
    slots,
    x_ref, sel_hbm, gate_hbm, up_ref, down_ref,
    y_ref,
    sel_ref, gate_ref, xall, wup, wdn, send, ret, pk, hid, dpk, yacc,
    sel_b, gate_b, code_s, rt_send, rt_recv, rowtab,
    in_sem, wup_sem, wdn_sem, ag_snd, ag_sem, sib_sem, rt_snd, rt_sem, snd_sem, rcv_sem,
):
    n_exp, cap = sel_ref.shape
    tok, width = x_ref.shape
    ff = up_ref.shape[2]
    nslot = NDEV * slots
    me = lax.axis_index("ep")
    core = me % 2
    sib = me + 1 - 2 * core
    xx = (me // 2) % 2
    yy = me // 4
    dx = 2 - 4 * xx
    dy = 4 - 8 * yy
    xn, yn, dg = me + dx, me + dy, me + dx + dy
    peers = (dg, sib + dx + dy, xn, sib + dx, yn, sib + dy, sib)
    ch = tok // CHUNKS
    half = CHUNKS // 2
    yorder = [*range(CHUNKS - 1, half - 1, -1), *range(half)]

    def remote(src, dst, ssem, rsem, dev):
        return pltpu.make_async_remote_copy(
            src_ref=src, dst_ref=dst, send_sem=ssem, recv_sem=rsem, device_id={"ep": dev}, device_id_type=MESH
        )

    def up_copy(e):
        return pltpu.make_async_copy(up_ref.at[e], wup.at[e % 2], wup_sem.at[e % 2])

    def down_copy(e):
        return pltpu.make_async_copy(down_ref.at[e], wdn.at[e % 2], wdn_sem.at[e % 2])

    own_copy = pltpu.make_async_copy(x_ref, xall.at[me], in_sem.at[2])
    own_copy.start()
    sel_copy = pltpu.make_async_copy(sel_hbm, sel_ref, in_sem.at[0])
    gate_copy = pltpu.make_async_copy(gate_hbm, gate_ref, in_sem.at[1])
    sel_copy.start()
    gate_copy.start()

    barrier = pltpu.get_barrier_semaphore()
    for dev in (sib, xn, yn):
        pl.semaphore_signal(barrier, inc=1, device_id={"ep": dev}, device_id_type=MESH)
    pl.semaphore_wait(barrier, 3)
    own_copy.wait()

    def piece(owner, c):
        return xall.at[owner, pl.ds(c * ch, ch), :]

    def take(ref, sem):
        pltpu.make_async_copy(ref, ref, sem).wait()

    def ag(owner, c, sem, dev):
        remote(piece(owner, c), piece(owner, c), ag_snd, sem, dev).start()

    for i in range(CHUNKS):
        ag(me, i, ag_sem.at[i], xn)
        ag(me, yorder[i], ag_sem.at[i], yn)
        ag(me, i, sib_sem.at[i // half], sib)

    for e in range(2):
        up_copy(e).start()
        down_copy(e).start()

    sel_copy.wait()
    gate_copy.wait()

    sel_cols = jnp.transpose(sel_ref[...].astype(F32)).astype(jnp.int32)
    gate_cols = jnp.transpose(gate_ref[...])
    for e in range(n_exp):
        sel_b[e * cap : (e + 1) * cap, :] = jnp.broadcast_to(sel_cols[:, e : e + 1], (cap, 128))
        gate_b[e * cap : (e + 1) * cap, :] = jnp.broadcast_to(gate_cols[:, e : e + 1], (cap, 128))
    upper = _onehot(_iota((cap, cap), 0) < _iota((cap, cap), 1))
    for e in range(n_exp):
        sel_row = sel_ref[pl.ds(e, 1), :]
        owner = lax.shift_right_logical(sel_row, 10)
        local = jnp.bitwise_and(sel_row, 1023)
        mine = jnp.broadcast_to(owner, (16, cap)) == _iota((16, cap), 0)
        cum = jnp.dot(_onehot(mine), upper, preferred_element_type=F32)
        rank = jnp.sum(jnp.where(mine, cum, 0.0), axis=0, keepdims=True)
        owner_f = owner.astype(F32)
        code_s[pl.ds(e, 1), :] = owner_f * slots + rank
        tcode = (owner_f * 128 + rank).astype(jnp.int32) + core * slots
        q = _onehot(jnp.broadcast_to(tcode, (NDEV * 128, cap)) == _iota((NDEV * 128, cap), 0))
        hi = lax.shift_right_logical(local, 5).astype(F32)
        lo = jnp.bitwise_and(local, 31).astype(F32)
        rows = _iota((16, cap), 0)
        lhs = jnp.where(rows == 0, hi, jnp.where(rows == 1, lo, jnp.where(rows == 2, 1.0, 0.0))).astype(BF16)
        t = lax.dot_general(lhs, q, (((1,), (1,)), ((), ())), preferred_element_type=F32)
        tab = t[0:1] * 32.0 + t[1:2] + t[2:3]
        for g in range(NDEV):
            rt_send[g, pl.ds(e, 1), :] = tab[:, g * 128 : (g + 1) * 128]
    rt_recv[me] = rt_send[me]
    yacc[...] = xall[me].astype(F32)
    def picks(rows, owner, first, depth):
        n = rows.size
        rel = sel_b[rows, :] - (owner * tok + first)
        lane = _iota((n, 128), 1)
        hot = jnp.concatenate([_onehot(rel == lane + g * 128) for g in range(depth // 128)], axis=1)
        return jnp.dot(hot, xall[owner, first : first + depth, :], preferred_element_type=F32)

    def gather(owner, first, depth, pairs=(0, n_exp // 2), fresh=False):
        n = 2 * cap

        def some(i, carry):
            rows = pl.ds(pl.multiple_of(i * n, n), n)
            got = picks(rows, owner, first, depth).astype(BF16)
            pk[rows, :] = got if fresh else pk[rows, :] + got
            return carry

        lax.fori_loop(*pairs, some, 0)

    def from_sib(group):
        take(xall.at[sib, pl.ds(0, half * ch), :], sib_sem.at[group])

    xs, ys, ds = sib + dx, sib + dy, sib + dx + dy
    hb = tok // 2

    def slot(i):
        take(xall.at[xn, pl.ds(0, 2 * ch), :], ag_sem.at[i])
        if i < CHUNKS:
            a, ca, b, cb = xn, i, yn, yorder[i]
        else:
            a, ca, b, cb = dg, i - CHUNKS, dg, yorder[i - CHUNKS]
        if i < half:
            ag(a, ca, ag_sem.at[CHUNKS + i], yn)
            ag(b, cb, ag_sem.at[CHUNKS + i], xn)
        ga = (2, 2, 2, 2, 4, 4, 5, 5, 6, 6, 7, 7)[i]
        gb = (3, 3, 3, 3, 4, 4, 5, 5, 6, 6, 7, 7)[i]
        ag(a, ca, sib_sem.at[ga], sib)
        ag(b, cb, sib_sem.at[gb], sib)

    def ret_copy(e, k):
        dev = peers[k]
        return remote(send.at[e, pl.ds(dev * slots, slots), :], ret.at[e, me], snd_sem, rcv_sem.at[e], dev)

    def loc_copy(e):
        return pltpu.make_async_copy(send.at[e, pl.ds(me * slots, slots), :], ret.at[e, me], rcv_sem.at[e])

    def up(lhs, m, e):
        up_copy(e).wait()
        tile = 1024

        def some(j, carry):
            cols = pl.ds(pl.multiple_of(j * tile, tile), tile)
            z = jnp.dot(lhs[...], wup[e % 2, :, cols], preferred_element_type=F32)
            hid[0:m, cols] = _gelu(z).astype(BF16)
            return carry

        lax.fori_loop(0, ff // tile, some, 0)

    def scatter(e, rows):
        code = code_s[pl.ds(e, 1), :].astype(jnp.int32)
        place = _onehot(jnp.broadcast_to(code, (nslot, cap)) == _iota((nslot, cap), 0))
        o = jnp.dot(hid[...], wdn[e % 2], preferred_element_type=F32)
        gate = jnp.concatenate([gate_b[rows, :]] * (width // 128), axis=1)
        contrib = (o * gate).astype(BF16)
        send[e] = jnp.dot(place, contrib, preferred_element_type=F32).astype(BF16)

    def early(e):
        rows = pl.ds(e * cap, cap)
        up(pk.at[rows, :], cap, e)
        down_copy(e).wait()
        scatter(e, rows)
        for k in range(2, NDEV - 1):
            ret_copy(e, k).start()
        loc_copy(e).start()

    def diagonal(e, carry):
        rows = pl.ds(pl.multiple_of(e * cap, cap), cap)
        m = 2 * slots
        base = pl.multiple_of((dg // 2) * m, m)
        code = code_s[pl.ds(e, 1), :].astype(jnp.int32) - base
        here = jnp.broadcast_to(code, (m, cap)) == _iota((m, cap), 0)
        gate = jnp.sum(jnp.where(here, gate_ref[pl.ds(e, 1), :], 0.0), axis=1, keepdims=True)
        dpk[...] = jnp.dot(_onehot(here), pk[rows, :], preferred_element_type=F32).astype(BF16)
        tile = 1024

        def some(j, c):
            cols = pl.ds(pl.multiple_of(j * tile, tile), tile)
            z = jnp.dot(dpk[...], wup[e % 2, :, cols], preferred_element_type=F32)
            hid[0:m, cols] = _gelu(z).astype(BF16)
            return c

        lax.fori_loop(0, ff // tile, some, 0)
        up_copy(e + 2).start()
        o = jnp.dot(hid[0:m, :], wdn[e % 2], preferred_element_type=F32)
        send[e, pl.ds(base, m), :] = (o * gate).astype(BF16)
        down_copy(e + 2).start()
        for k in range(2):
            ret_copy(e, k).start()
        return carry

    def produce(e):
        rows = pl.ds(pl.multiple_of(e * cap, cap), cap)
        up(pk.at[rows, :], cap, e)

        @pl.when(e + 2 < n_exp)
        def _():
            up_copy(e + 2).start()

        down_copy(e).wait()
        scatter(e, rows)

        @pl.when(e + 2 < n_exp)
        def _():
            down_copy(e + 2).start()

        for k in range(NDEV - 1):
            ret_copy(e, k).start()
        loc_copy(e).start()

    def arrived(e):
        take(ret.at[e], rcv_sem.at[e])

    def adds(e, j, tile):
        row = rowtab[pl.ds(e, 1), :].astype(jnp.int32)
        hot = _onehot(jnp.broadcast_to(row, (tile, nslot)) == _iota((tile, nslot), 0) + j * tile)
        return jnp.dot(hot, ret[e].reshape(nslot, width), preferred_element_type=F32)

    def combine(e):
        arrived(e)
        tile = 256

        def some(j, carry):
            rows = pl.ds(pl.multiple_of(j * tile, tile), tile)
            yacc[rows, :] += adds(e, j, tile)
            return carry

        lax.fori_loop(0, tok // tile, some, 0)

    qb = hb // 2
    gather(me, 0, hb, fresh=True)
    slot(0)
    gather(me, hb, hb)
    slot(1)
    from_sib(0)
    gather(sib, 0, hb)
    slot(2)
    from_sib(1)
    gather(sib, hb, hb)
    slot(3)
    gather(xn, 0, hb)
    from_sib(2)
    slot(4)
    for dev in peers:
        remote(rt_send.at[dev], rt_recv.at[me], rt_snd, rt_sem, dev).start()
    gather(yn, hb, hb)
    gather(xs, 0, hb)
    slot(5)
    from_sib(3)
    gather(ys, hb, hb)
    gather(xn, hb, qb)
    slot(6)
    gather(yn, 0, qb)
    from_sib(4)
    gather(xs, hb, qb)
    gather(ys, 0, qb)
    slot(7)
    first, later = (0, 1), (1, n_exp // 2)

    def third(pairs):
        gather(xn, hb + qb, qb, pairs)
        gather(yn, qb, qb, pairs)
        gather(xs, hb + qb, qb, pairs)
        gather(ys, qb, qb, pairs)

    from_sib(5)
    third(first)
    early(0)
    slot(8)
    early(1)
    slot(9)
    third(later)
    slot(10)
    from_sib(6)
    for dev in (dg, ds):
        gather(dev, 0, qb, first)
        gather(dev, tok - qb, qb, first)
    slot(11)
    from_sib(7)
    for dev in (dg, ds):
        gather(dev, qb, hb, first)

    lax.fori_loop(0, 2, diagonal, 0)

    take(rt_recv.at[pl.ds(0, NDEV - 1)], rt_sem)
    for p in range(NDEV // 2):
        rowtab[:, p * 128 : (p + 1) * 128] = rt_recv[2 * p] + rt_recv[2 * p + 1] - 1.0

    def pair(p, carry):
        for dev in (dg, ds):
            gather(dev, 0, tok, (p, p + 1))
        produce(2 * p)

        @pl.when(p >= 2)
        def _():
            combine(2 * p - 3)

        produce(2 * p + 1)
        combine(2 * p - 2)
        return carry

    lax.fori_loop(1, n_exp // 2, pair, 0)

    def rest(e, carry):
        combine(e)
        return carry

    lax.fori_loop(n_exp - 3, n_exp - 1, rest, 0)
    last = n_exp - 1
    arrived(last)
    tile = 256

    def finish(j, carry):
        rows = pl.ds(pl.multiple_of(j * tile, tile), tile)
        y_ref[rows, :] = (yacc[rows, :] + adds(last, j, tile)).astype(BF16)
        return carry

    lax.fori_loop(0, tok // tile, finish, 0)

    take(xall.at[pl.ds(0, 7)], ag_snd)
    take(rt_send.at[pl.ds(0, NDEV - 1)], rt_snd)
    take(send.at[pl.ds(0, n_exp * (NDEV - 1) // NDEV)], snd_sem)


def solution(mesh):
    def local_layer(x_loc, sel_loc, gate_loc, up_loc, down_loc):
        tok, width = x_loc.shape
        n_exp, cap = sel_loc.shape
        ff = up_loc.shape[2]
        slots = 2 * cap // NDEV
        nslot = NDEV * slots
        dma = pltpu.SemaphoreType.DMA
        vmem = pl.BlockSpec(memory_space=pltpu.VMEM)
        hbm = pl.BlockSpec(memory_space=pl.ANY)
        return pl.pallas_call(
            functools.partial(kernel, slots),
            out_shape=pltpu.VMEM((tok, width), BF16),
            in_specs=[hbm] * 5,
            out_specs=vmem,
            scratch_shapes=[
                pltpu.VMEM((n_exp, cap), jnp.int32),
                pltpu.VMEM((n_exp, cap), F32),
                pltpu.VMEM((NDEV, tok, width), BF16),
                pltpu.VMEM((2, width, ff), BF16),
                pltpu.VMEM((2, ff, width), BF16),
                pltpu.VMEM((n_exp, nslot, width), BF16),
                pltpu.VMEM((n_exp, NDEV, slots, width), BF16),
                pltpu.VMEM((n_exp * cap, width), BF16),
                pltpu.VMEM((cap, ff), BF16),
                pltpu.VMEM((2 * slots, width), BF16),
                pltpu.VMEM((tok, width), F32),
                pltpu.VMEM((n_exp * cap, 128), jnp.int32),
                pltpu.VMEM((n_exp * cap, 128), F32),
                pltpu.VMEM((n_exp, cap), F32),
                pltpu.VMEM((NDEV, n_exp, 128), F32),
                pltpu.VMEM((NDEV, n_exp, 128), F32),
                pltpu.VMEM((n_exp, nslot), F32),
                dma((3,)),
                dma((2,)),
                dma((2,)),
                dma,
                dma((CHUNKS + CHUNKS // 2,)),
                dma((8,)),
                dma,
                dma,
                dma,
                dma((n_exp,)),
            ],
            compiler_params=pltpu.CompilerParams(
                collective_id=0, has_side_effects=True, vmem_limit_bytes=64_000_000
            ),
            name="moe",
        )(x_loc, sel_loc, gate_loc, up_loc, down_loc)

    row_spec = P(("dp", "ep"), None)
    weight_spec = P("ep", None, None)
    return jax.shard_map(
        local_layer,
        mesh=mesh,
        in_specs=(row_spec, row_spec, row_spec, weight_spec, weight_spec),
        out_specs=row_spec,
        check_vma=False,
    )
```

```python
import functools

import jax
import jax.numpy as jnp
from jax import lax
from jax.experimental import pallas as pl
from jax.experimental.pallas import tpu as pltpu
from jax.sharding import PartitionSpec as P

F32 = jnp.float32
BF16 = jnp.bfloat16
MESH = pl.DeviceIdType.MESH

NDEV = 8
CHUNKS = 8


def _gelu(z):
    return 0.5 * z * (1.0 + jnp.tanh(0.7978845608028654 * (z + 0.044715 * (z * z * z))))


def _iota(shape, dim):
    return lax.broadcasted_iota(jnp.int32, shape, dim)


def _onehot(cond):
    return jnp.where(cond, 1.0, 0.0).astype(BF16)


def kernel(
    slots,
    x_ref, sel_hbm, gate_hbm, up_ref, down_ref,
    y_ref,
    sel_ref, gate_ref, xall, wup, wdn, send, ret, pk, hid, dpk, yacc,
    sel_b, gate_b, code_s, rt_send, rt_recv, rowtab,
    in_sem, wup_sem, wdn_sem, ag_snd, ag_sem, sib_sem, rt_snd, rt_sem, snd_sem, rcv_sem,
):
    n_exp, cap = sel_ref.shape
    tok, width = x_ref.shape
    ff = up_ref.shape[2]
    nslot = NDEV * slots
    me = lax.axis_index("ep")
    core = me % 2
    sib = me + 1 - 2 * core
    xx = (me // 2) % 2
    yy = me // 4
    dx = 2 - 4 * xx
    dy = 4 - 8 * yy
    xn, yn, dg = me + dx, me + dy, me + dx + dy
    peers = (dg, sib + dx + dy, xn, sib + dx, yn, sib + dy, sib)
    ch = tok // CHUNKS
    half = CHUNKS // 2
    yorder = [*range(CHUNKS - 1, half - 1, -1), *range(half)]

    def remote(src, dst, ssem, rsem, dev):
        return pltpu.make_async_remote_copy(
            src_ref=src, dst_ref=dst, send_sem=ssem, recv_sem=rsem, device_id={"ep": dev}, device_id_type=MESH
        )

    def up_copy(e):
        return pltpu.make_async_copy(up_ref.at[e], wup.at[e % 2], wup_sem.at[e % 2])

    def down_copy(e):
        return pltpu.make_async_copy(down_ref.at[e], wdn.at[e % 2], wdn_sem.at[e % 2])

    own_copy = pltpu.make_async_copy(x_ref, xall.at[me], in_sem.at[2])
    own_copy.start()
    sel_copy = pltpu.make_async_copy(sel_hbm, sel_ref, in_sem.at[0])
    gate_copy = pltpu.make_async_copy(gate_hbm, gate_ref, in_sem.at[1])
    sel_copy.start()
    gate_copy.start()

    barrier = pltpu.get_barrier_semaphore()
    for dev in (sib, xn, yn):
        pl.semaphore_signal(barrier, inc=1, device_id={"ep": dev}, device_id_type=MESH)
    pl.semaphore_wait(barrier, 3)
    own_copy.wait()

    def piece(owner, c):
        return xall.at[owner, pl.ds(c * ch, ch), :]

    def take(ref, sem):
        pltpu.make_async_copy(ref, ref, sem).wait()

    def ag(owner, c, sem, dev):
        remote(piece(owner, c), piece(owner, c), ag_snd, sem, dev).start()

    for i in range(CHUNKS):
        ag(me, i, ag_sem.at[i], xn)
        ag(me, yorder[i], ag_sem.at[i], yn)
        ag(me, i, sib_sem.at[i // half], sib)

    for e in range(2):
        up_copy(e).start()
        down_copy(e).start()

    sel_copy.wait()
    gate_copy.wait()

    sel_cols = jnp.transpose(sel_ref[...].astype(F32)).astype(jnp.int32)
    gate_cols = jnp.transpose(gate_ref[...])
    for e in range(n_exp):
        sel_b[e * cap : (e + 1) * cap, :] = jnp.broadcast_to(sel_cols[:, e : e + 1], (cap, 128))
        gate_b[e * cap : (e + 1) * cap, :] = jnp.broadcast_to(gate_cols[:, e : e + 1], (cap, 128))
    upper = _onehot(_iota((cap, cap), 0) < _iota((cap, cap), 1))
    for e in range(n_exp):
        sel_row = sel_ref[pl.ds(e, 1), :]
        owner = lax.shift_right_logical(sel_row, 10)
        local = jnp.bitwise_and(sel_row, 1023)
        mine = jnp.broadcast_to(owner, (16, cap)) == _iota((16, cap), 0)
        cum = jnp.dot(_onehot(mine), upper, preferred_element_type=F32)
        rank = jnp.sum(jnp.where(mine, cum, 0.0), axis=0, keepdims=True)
        owner_f = owner.astype(F32)
        code_s[pl.ds(e, 1), :] = owner_f * slots + rank
        tcode = (owner_f * 128 + rank).astype(jnp.int32) + core * slots
        q = _onehot(jnp.broadcast_to(tcode, (NDEV * 128, cap)) == _iota((NDEV * 128, cap), 0))
        hi = lax.shift_right_logical(local, 5).astype(F32)
        lo = jnp.bitwise_and(local, 31).astype(F32)
        rows = _iota((16, cap), 0)
        lhs = jnp.where(rows == 0, hi, jnp.where(rows == 1, lo, jnp.where(rows == 2, 1.0, 0.0))).astype(BF16)
        t = lax.dot_general(lhs, q, (((1,), (1,)), ((), ())), preferred_element_type=F32)
        tab = t[0:1] * 32.0 + t[1:2] + t[2:3]
        for g in range(NDEV):
            rt_send[g, pl.ds(e, 1), :] = tab[:, g * 128 : (g + 1) * 128]
    rt_recv[me] = rt_send[me]
    yacc[...] = xall[me].astype(F32)
    def picks(rows, owner, first, depth):
        n = rows.size
        rel = sel_b[rows, :] - (owner * tok + first)
        lane = _iota((n, 128), 1)
        hot = jnp.concatenate([_onehot(rel == lane + g * 128) for g in range(depth // 128)], axis=1)
        return jnp.dot(hot, xall[owner, first : first + depth, :], preferred_element_type=F32)

    def gather(owner, first, depth, pairs=(0, n_exp // 2), fresh=False):
        n = 2 * cap

        def some(i, carry):
            rows = pl.ds(pl.multiple_of(i * n, n), n)
            got = picks(rows, owner, first, depth).astype(BF16)
            pk[rows, :] = got if fresh else pk[rows, :] + got
            return carry

        lax.fori_loop(*pairs, some, 0)

    def from_sib(group):
        take(xall.at[sib, pl.ds(0, half * ch), :], sib_sem.at[group])

    xs, ys, ds = sib + dx, sib + dy, sib + dx + dy
    hb = tok // 2

    def slot(i):
        take(xall.at[xn, pl.ds(0, 2 * ch), :], ag_sem.at[i])
        if i < CHUNKS:
            a, ca, b, cb = xn, i, yn, yorder[i]
        else:
            a, ca, b, cb = dg, i - CHUNKS, dg, yorder[i - CHUNKS]
        if i < half:
            ag(a, ca, ag_sem.at[CHUNKS + i], yn)
            ag(b, cb, ag_sem.at[CHUNKS + i], xn)
        ga = (2, 2, 2, 2, 4, 4, 5, 5, 6, 6, 7, 7)[i]
        gb = (3, 3, 3, 3, 4, 4, 5, 5, 6, 6, 7, 7)[i]
        ag(a, ca, sib_sem.at[ga], sib)
        ag(b, cb, sib_sem.at[gb], sib)

    def ret_copy(e, k):
        dev = peers[k]
        return remote(send.at[e, pl.ds(dev * slots, slots), :], ret.at[e, me], snd_sem, rcv_sem.at[e], dev)

    last, hs = n_exp - 1, slots // 2

    def half_refs(dev, h):
        return send.at[last, pl.ds(dev * slots + h * hs, hs), :], ret.at[last, me, pl.ds(h * hs, hs), :]

    def loc_copy(e):
        return pltpu.make_async_copy(send.at[e, pl.ds(me * slots, slots), :], ret.at[e, me], rcv_sem.at[e])

    def up(lhs, m, e):
        up_copy(e).wait()
        tile = 1024

        def some(j, carry):
            cols = pl.ds(pl.multiple_of(j * tile, tile), tile)
            z = jnp.dot(lhs[...], wup[e % 2, :, cols], preferred_element_type=F32)
            hid[0:m, cols] = _gelu(z).astype(BF16)
            return carry

        lax.fori_loop(0, ff // tile, some, 0)

    def scatter(e, rows):
        code = code_s[pl.ds(e, 1), :].astype(jnp.int32)
        place = _onehot(jnp.broadcast_to(code, (nslot, cap)) == _iota((nslot, cap), 0))
        o = jnp.dot(hid[...], wdn[e % 2], preferred_element_type=F32)
        gate = jnp.concatenate([gate_b[rows, :]] * (width // 128), axis=1)
        contrib = (o * gate).astype(BF16)
        send[e] = jnp.dot(place, contrib, preferred_element_type=F32).astype(BF16)

    def early(e):
        rows = pl.ds(e * cap, cap)
        up(pk.at[rows, :], cap, e)
        down_copy(e).wait()
        scatter(e, rows)
        for k in range(2, NDEV - 1):
            ret_copy(e, k).start()
        loc_copy(e).start()

    def diagonal(e, carry):
        rows = pl.ds(pl.multiple_of(e * cap, cap), cap)
        m = 2 * slots
        base = pl.multiple_of((dg // 2) * m, m)
        code = code_s[pl.ds(e, 1), :].astype(jnp.int32) - base
        here = jnp.broadcast_to(code, (m, cap)) == _iota((m, cap), 0)
        gate = jnp.sum(jnp.where(here, gate_ref[pl.ds(e, 1), :], 0.0), axis=1, keepdims=True)
        dpk[...] = jnp.dot(_onehot(here), pk[rows, :], preferred_element_type=F32).astype(BF16)
        tile = 1024

        def some(j, c):
            cols = pl.ds(pl.multiple_of(j * tile, tile), tile)
            z = jnp.dot(dpk[...], wup[e % 2, :, cols], preferred_element_type=F32)
            hid[0:m, cols] = _gelu(z).astype(BF16)
            return c

        lax.fori_loop(0, ff // tile, some, 0)
        up_copy(e + 2).start()
        o = jnp.dot(hid[0:m, :], wdn[e % 2], preferred_element_type=F32)
        send[e, pl.ds(base, m), :] = (o * gate).astype(BF16)
        down_copy(e + 2).start()
        for k in range(2):
            ret_copy(e, k).start()
        return carry

    def produce(e):
        rows = pl.ds(pl.multiple_of(e * cap, cap), cap)
        up(pk.at[rows, :], cap, e)

        @pl.when(e + 2 < n_exp)
        def _():
            up_copy(e + 2).start()

        down_copy(e).wait()
        scatter(e, rows)

        @pl.when(e + 2 < n_exp)
        def _():
            down_copy(e + 2).start()

        @pl.when(e < last)
        def _():
            for k in range(NDEV - 1):
                ret_copy(e, k).start()
            loc_copy(e).start()

        @pl.when(e == last)
        def _():
            for h in range(2):
                for dev in peers:
                    src, dst = half_refs(dev, h)
                    remote(src, dst, snd_sem, rcv_sem.at[last + h], dev).start()
                src, dst = half_refs(me, h)
                pltpu.make_async_copy(src, dst, rcv_sem.at[last + h]).start()

    def arrived(e):
        take(ret.at[e], rcv_sem.at[e])

    def adds(e, j, tile):
        row = rowtab[pl.ds(e, 1), :].astype(jnp.int32)
        hot = _onehot(jnp.broadcast_to(row, (tile, nslot)) == _iota((tile, nslot), 0) + j * tile)
        return jnp.dot(hot, ret[e].reshape(nslot, width), preferred_element_type=F32)

    def combine(e):
        arrived(e)
        tile = 256

        def some(j, carry):
            rows = pl.ds(pl.multiple_of(j * tile, tile), tile)
            yacc[rows, :] += adds(e, j, tile)
            return carry

        lax.fori_loop(0, tok // tile, some, 0)

    qb = hb // 2
    gather(me, 0, hb, fresh=True)
    slot(0)
    gather(me, hb, hb)
    slot(1)
    from_sib(0)
    gather(sib, 0, hb)
    slot(2)
    from_sib(1)
    gather(sib, hb, hb)
    slot(3)
    gather(xn, 0, hb)
    from_sib(2)
    slot(4)
    for dev in peers:
        remote(rt_send.at[dev], rt_recv.at[me], rt_snd, rt_sem, dev).start()
    gather(yn, hb, hb)
    gather(xs, 0, hb)
    slot(5)
    from_sib(3)
    gather(ys, hb, hb)
    gather(xn, hb, qb)
    slot(6)
    gather(yn, 0, qb)
    from_sib(4)
    gather(xs, hb, qb)
    gather(ys, 0, qb)
    slot(7)
    first, later = (0, 1), (1, n_exp // 2)

    def third(pairs):
        gather(xn, hb + qb, qb, pairs)
        gather(yn, qb, qb, pairs)
        gather(xs, hb + qb, qb, pairs)
        gather(ys, qb, qb, pairs)

    from_sib(5)
    third(first)
    early(0)
    slot(8)
    early(1)
    slot(9)
    third(later)
    slot(10)
    from_sib(6)
    for dev in (dg, ds):
        gather(dev, 0, qb, first)
        gather(dev, tok - qb, qb, first)
    slot(11)
    from_sib(7)
    for dev in (dg, ds):
        gather(dev, qb, hb, first)

    lax.fori_loop(0, 2, diagonal, 0)

    take(rt_recv.at[pl.ds(0, NDEV - 1)], rt_sem)
    for p in range(NDEV // 2):
        rowtab[:, p * 128 : (p + 1) * 128] = rt_recv[2 * p] + rt_recv[2 * p + 1] - 1.0

    def pair(p, carry):
        for dev in (dg, ds):
            gather(dev, 0, tok, (p, p + 1))
        produce(2 * p)

        @pl.when(p >= 2)
        def _():
            combine(2 * p - 3)

        produce(2 * p + 1)
        combine(2 * p - 2)
        return carry

    lax.fori_loop(1, n_exp // 2, pair, 0)

    def rest(e, carry):
        combine(e)
        return carry

    lax.fori_loop(n_exp - 3, n_exp - 1, rest, 0)
    row = rowtab[pl.ds(last, 1), :].astype(jnp.int32)
    for h in range(2):
        picks_h = [row[:, d * slots + h * hs : d * slots + (h + 1) * hs] for d in range(NDEV)]
        lanes = jnp.concatenate(picks_h, axis=1)
        take(ret.at[last, pl.ds(0, NDEV // 2)], rcv_sem.at[last + h])
        tile = 512
        for j in range(tok // tile):
            rows = pl.ds(j * tile, tile)
            hot = _onehot(jnp.broadcast_to(lanes, (tile, nslot // 2)) == _iota((tile, nslot // 2), 0) + j * tile)
            back = ret[last, :, h * hs : (h + 1) * hs, :].reshape(nslot // 2, width)
            total = yacc[rows, :] + jnp.dot(hot, back, preferred_element_type=F32)
            if h == 0:
                yacc[rows, :] = total
            else:
                y_ref[rows, :] = total.astype(BF16)

    take(xall.at[pl.ds(0, 7)], ag_snd)
    take(rt_send.at[pl.ds(0, NDEV - 1)], rt_snd)
    take(send.at[pl.ds(0, n_exp * (NDEV - 1) // NDEV)], snd_sem)


def solution(mesh):
    def local_layer(x_loc, sel_loc, gate_loc, up_loc, down_loc):
        tok, width = x_loc.shape
        n_exp, cap = sel_loc.shape
        ff = up_loc.shape[2]
        slots = 2 * cap // NDEV
        nslot = NDEV * slots
        dma = pltpu.SemaphoreType.DMA
        vmem = pl.BlockSpec(memory_space=pltpu.VMEM)
        hbm = pl.BlockSpec(memory_space=pl.ANY)
        return pl.pallas_call(
            functools.partial(kernel, slots),
            out_shape=pltpu.VMEM((tok, width), BF16),
            in_specs=[hbm] * 5,
            out_specs=vmem,
            scratch_shapes=[
                pltpu.VMEM((n_exp, cap), jnp.int32),
                pltpu.VMEM((n_exp, cap), F32),
                pltpu.VMEM((NDEV, tok, width), BF16),
                pltpu.VMEM((2, width, ff), BF16),
                pltpu.VMEM((2, ff, width), BF16),
                pltpu.VMEM((n_exp, nslot, width), BF16),
                pltpu.VMEM((n_exp, NDEV, slots, width), BF16),
                pltpu.VMEM((n_exp * cap, width), BF16),
                pltpu.VMEM((cap, ff), BF16),
                pltpu.VMEM((2 * slots, width), BF16),
                pltpu.VMEM((tok, width), F32),
                pltpu.VMEM((n_exp * cap, 128), jnp.int32),
                pltpu.VMEM((n_exp * cap, 128), F32),
                pltpu.VMEM((n_exp, cap), F32),
                pltpu.VMEM((NDEV, n_exp, 128), F32),
                pltpu.VMEM((NDEV, n_exp, 128), F32),
                pltpu.VMEM((n_exp, nslot), F32),
                dma((3,)),
                dma((2,)),
                dma((2,)),
                dma,
                dma((CHUNKS + CHUNKS // 2,)),
                dma((8,)),
                dma,
                dma,
                dma,
                dma((n_exp + 1,)),
            ],
            compiler_params=pltpu.CompilerParams(
                collective_id=0, has_side_effects=True, vmem_limit_bytes=64_000_000
            ),
            name="moe",
        )(x_loc, sel_loc, gate_loc, up_loc, down_loc)

    row_spec = P(("dp", "ep"), None)
    weight_spec = P("ep", None, None)
    return jax.shard_map(
        local_layer,
        mesh=mesh,
        in_specs=(row_spec, row_spec, row_spec, weight_spec, weight_spec),
        out_specs=row_spec,
        check_vma=False,
    )
```

```python
import functools

import jax
import jax.numpy as jnp
from jax import lax
from jax.experimental import pallas as pl
from jax.experimental.pallas import tpu as pltpu
from jax.sharding import PartitionSpec as P

F32 = jnp.float32
BF16 = jnp.bfloat16
MESH = pl.DeviceIdType.MESH

NDEV = 8
CHUNKS = 8


def _gelu(z):
    return 0.5 * z * (1.0 + jnp.tanh(0.7978845608028654 * (z + 0.044715 * (z * z * z))))


def _iota(shape, dim):
    return lax.broadcasted_iota(jnp.int32, shape, dim)


def _onehot(cond):
    return jnp.where(cond, 1.0, 0.0).astype(BF16)


def kernel(
    slots,
    x_ref, sel_hbm, gate_hbm, up_ref, down_ref,
    y_ref,
    sel_ref, gate_ref, xall, wup, wdn, send, ret, pk, hid, dpk, yacc,
    sel_b, gate_b, code_s, rt_send, rt_recv, rowtab,
    in_sem, wup_sem, wdn_sem, ag_snd, ag_sem, sib_sem, rt_snd, rt_sem, snd_sem, rcv_sem,
):
    n_exp, cap = sel_ref.shape
    tok, width = x_ref.shape
    ff = up_ref.shape[2]
    nslot = NDEV * slots
    me = lax.axis_index("ep")
    core = me % 2
    sib = me + 1 - 2 * core
    xx = (me // 2) % 2
    yy = me // 4
    dx = 2 - 4 * xx
    dy = 4 - 8 * yy
    xn, yn, dg = me + dx, me + dy, me + dx + dy
    peers = (dg, sib + dx + dy, xn, sib + dx, yn, sib + dy, sib)
    ch = tok // CHUNKS
    half = CHUNKS // 2
    yorder = [*range(CHUNKS - 1, half - 1, -1), *range(half)]

    def remote(src, dst, ssem, rsem, dev):
        return pltpu.make_async_remote_copy(
            src_ref=src, dst_ref=dst, send_sem=ssem, recv_sem=rsem, device_id={"ep": dev}, device_id_type=MESH
        )

    def up_copy(e):
        return pltpu.make_async_copy(up_ref.at[e], wup.at[e % 2], wup_sem.at[e % 2])

    def down_copy(e):
        return pltpu.make_async_copy(down_ref.at[e], wdn.at[e % 2], wdn_sem.at[e % 2])

    own_copy = pltpu.make_async_copy(x_ref, xall.at[me], in_sem.at[2])
    own_copy.start()
    sel_copy = pltpu.make_async_copy(sel_hbm, sel_ref, in_sem.at[0])
    gate_copy = pltpu.make_async_copy(gate_hbm, gate_ref, in_sem.at[1])
    sel_copy.start()
    gate_copy.start()

    barrier = pltpu.get_barrier_semaphore()
    for dev in (sib, xn, yn):
        pl.semaphore_signal(barrier, inc=1, device_id={"ep": dev}, device_id_type=MESH)
    pl.semaphore_wait(barrier, 3)
    own_copy.wait()

    def piece(owner, c):
        return xall.at[owner, pl.ds(c * ch, ch), :]

    def take(ref, sem):
        pltpu.make_async_copy(ref, ref, sem).wait()

    def ag(owner, c, sem, dev):
        remote(piece(owner, c), piece(owner, c), ag_snd, sem, dev).start()

    for i in range(CHUNKS):
        ag(me, i, ag_sem.at[i], xn)
        ag(me, yorder[i], ag_sem.at[i], yn)
        ag(me, i, sib_sem.at[i // half], sib)

    for e in range(2):
        up_copy(e).start()
        down_copy(e).start()

    sel_copy.wait()
    gate_copy.wait()

    sel_cols = jnp.transpose(sel_ref[...].astype(F32)).astype(jnp.int32)
    gate_cols = jnp.transpose(gate_ref[...])
    for e in range(n_exp):
        sel_b[e * cap : (e + 1) * cap, :] = jnp.broadcast_to(sel_cols[:, e : e + 1], (cap, 128))
        gate_b[e * cap : (e + 1) * cap, :] = jnp.broadcast_to(gate_cols[:, e : e + 1], (cap, 128))
    upper = _onehot(_iota((cap, cap), 0) < _iota((cap, cap), 1))
    for e in range(n_exp):
        sel_row = sel_ref[pl.ds(e, 1), :]
        owner = lax.shift_right_logical(sel_row, 10)
        local = jnp.bitwise_and(sel_row, 1023)
        mine = jnp.broadcast_to(owner, (16, cap)) == _iota((16, cap), 0)
        cum = jnp.dot(_onehot(mine), upper, preferred_element_type=F32)
        rank = jnp.sum(jnp.where(mine, cum, 0.0), axis=0, keepdims=True)
        owner_f = owner.astype(F32)
        code_s[pl.ds(e, 1), :] = owner_f * slots + rank
        tcode = (owner_f * 128 + rank).astype(jnp.int32) + core * slots
        q = _onehot(jnp.broadcast_to(tcode, (NDEV * 128, cap)) == _iota((NDEV * 128, cap), 0))
        hi = lax.shift_right_logical(local, 5).astype(F32)
        lo = jnp.bitwise_and(local, 31).astype(F32)
        rows = _iota((16, cap), 0)
        lhs = jnp.where(rows == 0, hi, jnp.where(rows == 1, lo, jnp.where(rows == 2, 1.0, 0.0))).astype(BF16)
        t = lax.dot_general(lhs, q, (((1,), (1,)), ((), ())), preferred_element_type=F32)
        tab = t[0:1] * 32.0 + t[1:2] + t[2:3]
        for g in range(NDEV):
            rt_send[g, pl.ds(e, 1), :] = tab[:, g * 128 : (g + 1) * 128]
    rt_recv[me] = rt_send[me]
    yacc[...] = xall[me].astype(F32)
    def picks(rows, owner, first, depth):
        n = rows.size
        rel = sel_b[rows, :] - (owner * tok + first)
        lane = _iota((n, 128), 1)
        hot = jnp.concatenate([_onehot(rel == lane + g * 128) for g in range(depth // 128)], axis=1)
        return jnp.dot(hot, xall[owner, first : first + depth, :], preferred_element_type=F32)

    def gather(owner, first, depth, pairs=(0, n_exp // 2), fresh=False):
        n = 2 * cap

        def some(i, carry):
            rows = pl.ds(pl.multiple_of(i * n, n), n)
            got = picks(rows, owner, first, depth).astype(BF16)
            pk[rows, :] = got if fresh else pk[rows, :] + got
            return carry

        lax.fori_loop(*pairs, some, 0)

    def from_sib(group):
        take(xall.at[sib, pl.ds(0, half * ch), :], sib_sem.at[group])

    xs, ys, ds = sib + dx, sib + dy, sib + dx + dy
    hb = tok // 2

    def slot(i):
        take(xall.at[xn, pl.ds(0, 2 * ch), :], ag_sem.at[i])
        if i < CHUNKS:
            a, ca, b, cb = xn, i, yn, yorder[i]
        else:
            a, ca, b, cb = dg, i - CHUNKS, dg, yorder[i - CHUNKS]
        if i < half:
            ag(a, ca, ag_sem.at[CHUNKS + i], yn)
            ag(b, cb, ag_sem.at[CHUNKS + i], xn)
        ga = (2, 2, 2, 2, 4, 4, 5, 5, 6, 6, 7, 7)[i]
        gb = (3, 3, 3, 3, 4, 4, 5, 5, 6, 6, 7, 7)[i]
        ag(a, ca, sib_sem.at[ga], sib)
        ag(b, cb, sib_sem.at[gb], sib)

    def ret_copy(e, k):
        dev = peers[k]
        return remote(send.at[e, pl.ds(dev * slots, slots), :], ret.at[e, me], snd_sem, rcv_sem.at[e], dev)

    last, hs = n_exp - 1, slots // 2
    spread = (2, 0, 4, 3, 1, 5, 6)

    def half_refs(dev, h):
        return send.at[last, pl.ds(dev * slots + h * hs, hs), :], ret.at[last, me, pl.ds(h * hs, hs), :]

    def loc_copy(e):
        return pltpu.make_async_copy(send.at[e, pl.ds(me * slots, slots), :], ret.at[e, me], rcv_sem.at[e])

    def up(lhs, m, e):
        up_copy(e).wait()
        tile = 1024

        def some(j, carry):
            cols = pl.ds(pl.multiple_of(j * tile, tile), tile)
            z = jnp.dot(lhs[...], wup[e % 2, :, cols], preferred_element_type=F32)
            hid[0:m, cols] = _gelu(z).astype(BF16)
            return carry

        lax.fori_loop(0, ff // tile, some, 0)

    def scatter(e, rows):
        code = code_s[pl.ds(e, 1), :].astype(jnp.int32)
        place = _onehot(jnp.broadcast_to(code, (nslot, cap)) == _iota((nslot, cap), 0))
        o = jnp.dot(hid[...], wdn[e % 2], preferred_element_type=F32)
        gate = jnp.concatenate([gate_b[rows, :]] * (width // 128), axis=1)
        contrib = (o * gate).astype(BF16)
        send[e] = jnp.dot(place, contrib, preferred_element_type=F32).astype(BF16)

    def early(e):
        rows = pl.ds(e * cap, cap)
        up(pk.at[rows, :], cap, e)
        down_copy(e).wait()
        scatter(e, rows)
        for k in range(2, NDEV - 1):
            ret_copy(e, k).start()
        loc_copy(e).start()

    def diagonal(e, carry):
        rows = pl.ds(pl.multiple_of(e * cap, cap), cap)
        m = 2 * slots
        base = pl.multiple_of((dg // 2) * m, m)
        code = code_s[pl.ds(e, 1), :].astype(jnp.int32) - base
        here = jnp.broadcast_to(code, (m, cap)) == _iota((m, cap), 0)
        gate = jnp.sum(jnp.where(here, gate_ref[pl.ds(e, 1), :], 0.0), axis=1, keepdims=True)
        dpk[...] = jnp.dot(_onehot(here), pk[rows, :], preferred_element_type=F32).astype(BF16)
        tile = 1024

        def some(j, c):
            cols = pl.ds(pl.multiple_of(j * tile, tile), tile)
            z = jnp.dot(dpk[...], wup[e % 2, :, cols], preferred_element_type=F32)
            hid[0:m, cols] = _gelu(z).astype(BF16)
            return c

        lax.fori_loop(0, ff // tile, some, 0)
        up_copy(e + 2).start()
        o = jnp.dot(hid[0:m, :], wdn[e % 2], preferred_element_type=F32)
        send[e, pl.ds(base, m), :] = (o * gate).astype(BF16)
        down_copy(e + 2).start()
        for k in range(2):
            ret_copy(e, k).start()
        return carry

    def produce(e):
        rows = pl.ds(pl.multiple_of(e * cap, cap), cap)
        up(pk.at[rows, :], cap, e)

        @pl.when(e + 2 < n_exp)
        def _():
            up_copy(e + 2).start()

        down_copy(e).wait()
        scatter(e, rows)

        @pl.when(e + 2 < n_exp)
        def _():
            down_copy(e + 2).start()

        @pl.when(e < last)
        def _():
            for k in spread:
                ret_copy(e, k).start()
            loc_copy(e).start()

        @pl.when(e == last)
        def _():
            for h in range(2):
                for dev in [peers[k] for k in spread]:
                    src, dst = half_refs(dev, h)
                    remote(src, dst, snd_sem, rcv_sem.at[last + h], dev).start()
                src, dst = half_refs(me, h)
                pltpu.make_async_copy(src, dst, rcv_sem.at[last + h]).start()

    def arrived(e):
        take(ret.at[e], rcv_sem.at[e])

    def adds(e, j, tile):
        row = rowtab[pl.ds(e, 1), :].astype(jnp.int32)
        hot = _onehot(jnp.broadcast_to(row, (tile, nslot)) == _iota((tile, nslot), 0) + j * tile)
        return jnp.dot(hot, ret[e].reshape(nslot, width), preferred_element_type=F32)

    def combine(e):
        arrived(e)
        tile = 256

        def some(j, carry):
            rows = pl.ds(pl.multiple_of(j * tile, tile), tile)
            yacc[rows, :] += adds(e, j, tile)
            return carry

        lax.fori_loop(0, tok // tile, some, 0)

    qb = hb // 2
    gather(me, 0, hb, fresh=True)
    slot(0)
    gather(me, hb, hb)
    slot(1)
    from_sib(0)
    gather(sib, 0, hb)
    slot(2)
    from_sib(1)
    gather(sib, hb, hb)
    slot(3)
    gather(xn, 0, hb)
    from_sib(2)
    slot(4)
    for dev in peers:
        remote(rt_send.at[dev], rt_recv.at[me], rt_snd, rt_sem, dev).start()
    gather(yn, hb, hb)
    gather(xs, 0, hb)
    slot(5)
    from_sib(3)
    gather(ys, hb, hb)
    gather(xn, hb, qb)
    slot(6)
    gather(yn, 0, qb)
    from_sib(4)
    gather(xs, hb, qb)
    gather(ys, 0, qb)
    slot(7)
    first, later = (0, 1), (1, n_exp // 2)

    def third(pairs):
        gather(xn, hb + qb, qb, pairs)
        gather(yn, qb, qb, pairs)
        gather(xs, hb + qb, qb, pairs)
        gather(ys, qb, qb, pairs)

    from_sib(5)
    third(first)
    early(0)
    slot(8)
    early(1)
    slot(9)
    third(later)
    slot(10)
    from_sib(6)
    for dev in (dg, ds):
        gather(dev, 0, qb, first)
        gather(dev, tok - qb, qb, first)
    slot(11)
    from_sib(7)
    for dev in (dg, ds):
        gather(dev, qb, hb, first)

    lax.fori_loop(0, 2, diagonal, 0)

    take(rt_recv.at[pl.ds(0, NDEV - 1)], rt_sem)
    for p in range(NDEV // 2):
        rowtab[:, p * 128 : (p + 1) * 128] = rt_recv[2 * p] + rt_recv[2 * p + 1] - 1.0

    def pair(p, carry):
        for dev in (dg, ds):
            gather(dev, 0, tok, (p, p + 1))
        produce(2 * p)

        @pl.when(p >= 2)
        def _():
            combine(2 * p - 3)

        produce(2 * p + 1)
        combine(2 * p - 2)
        return carry

    lax.fori_loop(1, n_exp // 2, pair, 0)

    def rest(e, carry):
        combine(e)
        return carry

    lax.fori_loop(n_exp - 3, n_exp - 1, rest, 0)
    row = rowtab[pl.ds(last, 1), :].astype(jnp.int32)
    for h in range(2):
        picks_h = [row[:, d * slots + h * hs : d * slots + (h + 1) * hs] for d in range(NDEV)]
        lanes = jnp.concatenate(picks_h, axis=1)
        take(ret.at[last, pl.ds(0, NDEV // 2)], rcv_sem.at[last + h])
        tile = 512
        for j in range(tok // tile):
            rows = pl.ds(j * tile, tile)
            hot = _onehot(jnp.broadcast_to(lanes, (tile, nslot // 2)) == _iota((tile, nslot // 2), 0) + j * tile)
            back = ret[last, :, h * hs : (h + 1) * hs, :].reshape(nslot // 2, width)
            total = yacc[rows, :] + jnp.dot(hot, back, preferred_element_type=F32)
            if h == 0:
                yacc[rows, :] = total
            else:
                y_ref[rows, :] = total.astype(BF16)

    take(xall.at[pl.ds(0, 7)], ag_snd)
    take(rt_send.at[pl.ds(0, NDEV - 1)], rt_snd)
    take(send.at[pl.ds(0, n_exp * (NDEV - 1) // NDEV)], snd_sem)


def solution(mesh):
    def local_layer(x_loc, sel_loc, gate_loc, up_loc, down_loc):
        tok, width = x_loc.shape
        n_exp, cap = sel_loc.shape
        ff = up_loc.shape[2]
        slots = 2 * cap // NDEV
        nslot = NDEV * slots
        dma = pltpu.SemaphoreType.DMA
        vmem = pl.BlockSpec(memory_space=pltpu.VMEM)
        hbm = pl.BlockSpec(memory_space=pl.ANY)
        return pl.pallas_call(
            functools.partial(kernel, slots),
            out_shape=pltpu.VMEM((tok, width), BF16),
            in_specs=[hbm] * 5,
            out_specs=vmem,
            scratch_shapes=[
                pltpu.VMEM((n_exp, cap), jnp.int32),
                pltpu.VMEM((n_exp, cap), F32),
                pltpu.VMEM((NDEV, tok, width), BF16),
                pltpu.VMEM((2, width, ff), BF16),
                pltpu.VMEM((2, ff, width), BF16),
                pltpu.VMEM((n_exp, nslot, width), BF16),
                pltpu.VMEM((n_exp, NDEV, slots, width), BF16),
                pltpu.VMEM((n_exp * cap, width), BF16),
                pltpu.VMEM((cap, ff), BF16),
                pltpu.VMEM((2 * slots, width), BF16),
                pltpu.VMEM((tok, width), F32),
                pltpu.VMEM((n_exp * cap, 128), jnp.int32),
                pltpu.VMEM((n_exp * cap, 128), F32),
                pltpu.VMEM((n_exp, cap), F32),
                pltpu.VMEM((NDEV, n_exp, 128), F32),
                pltpu.VMEM((NDEV, n_exp, 128), F32),
                pltpu.VMEM((n_exp, nslot), F32),
                dma((3,)),
                dma((2,)),
                dma((2,)),
                dma,
                dma((CHUNKS + CHUNKS // 2,)),
                dma((8,)),
                dma,
                dma,
                dma,
                dma((n_exp + 1,)),
            ],
            compiler_params=pltpu.CompilerParams(
                collective_id=0, has_side_effects=True, vmem_limit_bytes=64_000_000
            ),
            name="moe",
        )(x_loc, sel_loc, gate_loc, up_loc, down_loc)

    row_spec = P(("dp", "ep"), None)
    weight_spec = P("ep", None, None)
    return jax.shard_map(
        local_layer,
        mesh=mesh,
        in_specs=(row_spec, row_spec, row_spec, weight_spec, weight_spec),
        out_specs=row_spec,
        check_vma=False,
    )
```

```python
import functools

import jax
import jax.numpy as jnp
from jax import lax
from jax.experimental import pallas as pl
from jax.experimental.pallas import tpu as pltpu
from jax.sharding import PartitionSpec as P

F32 = jnp.float32
BF16 = jnp.bfloat16
MESH = pl.DeviceIdType.MESH

NDEV = 8
CHUNKS = 8


def _gelu(z):
    return 0.5 * z * (1.0 + jnp.tanh(0.7978845608028654 * (z + 0.044715 * (z * z * z))))


def _iota(shape, dim):
    return lax.broadcasted_iota(jnp.int32, shape, dim)


def _onehot(cond):
    return jnp.where(cond, 1.0, 0.0).astype(BF16)


def kernel(
    slots,
    x_ref, sel_hbm, gate_hbm, up_ref, down_ref,
    y_ref,
    sel_ref, gate_ref, xall, wup, wdn, send, ret, pk, hid, dpk, yacc,
    sel_b, gate_b, code_s, rt_send, rt_recv, rowtab,
    in_sem, wup_sem, wdn_sem, ag_snd, ag_sem, sib_sem, rt_snd, rt_sem, snd_sem, rcv_sem,
):
    n_exp, cap = sel_ref.shape
    tok, width = x_ref.shape
    ff = up_ref.shape[2]
    nslot = NDEV * slots
    me = lax.axis_index("ep")
    core = me % 2
    sib = me + 1 - 2 * core
    xx = (me // 2) % 2
    yy = me // 4
    dx = 2 - 4 * xx
    dy = 4 - 8 * yy
    xn, yn, dg = me + dx, me + dy, me + dx + dy
    peers = (dg, sib + dx + dy, xn, sib + dx, yn, sib + dy, sib)
    ch = tok // CHUNKS
    half = CHUNKS // 2
    yorder = [*range(CHUNKS - 1, half - 1, -1), *range(half)]

    def remote(src, dst, ssem, rsem, dev):
        return pltpu.make_async_remote_copy(
            src_ref=src, dst_ref=dst, send_sem=ssem, recv_sem=rsem, device_id={"ep": dev}, device_id_type=MESH
        )

    def up_copy(e):
        return pltpu.make_async_copy(up_ref.at[e], wup.at[e % 2], wup_sem.at[e % 2])

    def down_copy(e):
        return pltpu.make_async_copy(down_ref.at[e], wdn.at[e % 2], wdn_sem.at[e % 2])

    own_copy = pltpu.make_async_copy(x_ref, xall.at[me], in_sem.at[2])
    own_copy.start()
    sel_copy = pltpu.make_async_copy(sel_hbm, sel_ref, in_sem.at[0])
    gate_copy = pltpu.make_async_copy(gate_hbm, gate_ref, in_sem.at[1])
    sel_copy.start()
    gate_copy.start()

    barrier = pltpu.get_barrier_semaphore()
    for dev in (sib, xn, yn):
        pl.semaphore_signal(barrier, inc=1, device_id={"ep": dev}, device_id_type=MESH)
    pl.semaphore_wait(barrier, 3)
    own_copy.wait()

    def piece(owner, c):
        return xall.at[owner, pl.ds(c * ch, ch), :]

    def take(ref, sem):
        pltpu.make_async_copy(ref, ref, sem).wait()

    def ag(owner, c, sem, dev):
        remote(piece(owner, c), piece(owner, c), ag_snd, sem, dev).start()

    for i in range(CHUNKS):
        ag(me, i, ag_sem.at[i], xn)
        ag(me, yorder[i], ag_sem.at[i], yn)
        ag(me, i, sib_sem.at[i // half], sib)

    for e in range(2):
        up_copy(e).start()
        down_copy(e).start()

    sel_copy.wait()
    gate_copy.wait()

    sel_cols = jnp.transpose(sel_ref[...].astype(F32)).astype(jnp.int32)
    gate_cols = jnp.transpose(gate_ref[...])
    for e in range(n_exp):
        sel_b[e * cap : (e + 1) * cap, :] = jnp.broadcast_to(sel_cols[:, e : e + 1], (cap, 128))
        gate_b[e * cap : (e + 1) * cap, :] = jnp.broadcast_to(gate_cols[:, e : e + 1], (cap, 128))
    upper = _onehot(_iota((cap, cap), 0) < _iota((cap, cap), 1))
    for e in range(n_exp):
        sel_row = sel_ref[pl.ds(e, 1), :]
        owner = lax.shift_right_logical(sel_row, 10)
        local = jnp.bitwise_and(sel_row, 1023)
        mine = jnp.broadcast_to(owner, (16, cap)) == _iota((16, cap), 0)
        cum = jnp.dot(_onehot(mine), upper, preferred_element_type=F32)
        rank = jnp.sum(jnp.where(mine, cum, 0.0), axis=0, keepdims=True)
        owner_f = owner.astype(F32)
        code_s[pl.ds(e, 1), :] = owner_f * slots + rank
        tcode = (owner_f * 128 + rank).astype(jnp.int32) + core * slots
        q = _onehot(jnp.broadcast_to(tcode, (NDEV * 128, cap)) == _iota((NDEV * 128, cap), 0))
        hi = lax.shift_right_logical(local, 5).astype(F32)
        lo = jnp.bitwise_and(local, 31).astype(F32)
        rows = _iota((16, cap), 0)
        lhs = jnp.where(rows == 0, hi, jnp.where(rows == 1, lo, jnp.where(rows == 2, 1.0, 0.0))).astype(BF16)
        t = lax.dot_general(lhs, q, (((1,), (1,)), ((), ())), preferred_element_type=F32)
        tab = t[0:1] * 32.0 + t[1:2] + t[2:3]
        for g in range(NDEV):
            rt_send[g, pl.ds(e, 1), :] = tab[:, g * 128 : (g + 1) * 128]
    rt_recv[me] = rt_send[me]
    yacc[...] = xall[me].astype(F32)
    def picks(rows, owner, first, depth):
        n = rows.size
        rel = sel_b[rows, :] - (owner * tok + first)
        lane = _iota((n, 128), 1)
        hot = jnp.concatenate([_onehot(rel == lane + g * 128) for g in range(depth // 128)], axis=1)
        return jnp.dot(hot, xall[owner, first : first + depth, :], preferred_element_type=F32)

    def gather(owner, first, depth, pairs=(0, n_exp // 2), fresh=False):
        n = 2 * cap

        def some(i, carry):
            rows = pl.ds(pl.multiple_of(i * n, n), n)
            got = picks(rows, owner, first, depth).astype(BF16)
            pk[rows, :] = got if fresh else pk[rows, :] + got
            return carry

        lax.fori_loop(*pairs, some, 0)

    def from_sib(group):
        take(xall.at[sib, pl.ds(0, half * ch), :], sib_sem.at[group])

    xs, ys, ds = sib + dx, sib + dy, sib + dx + dy
    hb = tok // 2

    def slot(i):
        take(xall.at[xn, pl.ds(0, 2 * ch), :], ag_sem.at[i])
        if i < CHUNKS:
            a, ca, b, cb = xn, i, yn, yorder[i]
        else:
            a, ca, b, cb = dg, i - CHUNKS, dg, yorder[i - CHUNKS]
        if i < half:
            ag(a, ca, ag_sem.at[CHUNKS + i], yn)
            ag(b, cb, ag_sem.at[CHUNKS + i], xn)
        ga = (2, 2, 2, 2, 4, 4, 5, 5, 6, 6, 7, 7)[i]
        gb = (3, 3, 3, 3, 4, 4, 5, 5, 6, 6, 7, 7)[i]
        ag(a, ca, sib_sem.at[ga], sib)
        ag(b, cb, sib_sem.at[gb], sib)

    def ret_copy(e, k):
        dev = peers[k]
        return remote(send.at[e, pl.ds(dev * slots, slots), :], ret.at[e, me], snd_sem, rcv_sem.at[e], dev)

    last, hs = n_exp - 1, slots // 2
    spread = (2, 0, 4, 3, 1, 5, 6)

    def half_refs(dev, h):
        return send.at[last, pl.ds(dev * slots + h * hs, hs), :], ret.at[last, me, pl.ds(h * hs, hs), :]

    def loc_copy(e):
        return pltpu.make_async_copy(send.at[e, pl.ds(me * slots, slots), :], ret.at[e, me], rcv_sem.at[e])

    def up(lhs, m, e):
        up_copy(e).wait()
        tile = 1024

        def some(j, carry):
            cols = pl.ds(pl.multiple_of(j * tile, tile), tile)
            z = jnp.dot(lhs[...], wup[e % 2, :, cols], preferred_element_type=F32)
            hid[0:m, cols] = _gelu(z).astype(BF16)
            return carry

        lax.fori_loop(0, ff // tile, some, 0)

    def scatter(e, rows):
        code = code_s[pl.ds(e, 1), :].astype(jnp.int32)
        place = _onehot(jnp.broadcast_to(code, (nslot, cap)) == _iota((nslot, cap), 0))
        o = jnp.dot(hid[...], wdn[e % 2], preferred_element_type=F32)
        gate = jnp.concatenate([gate_b[rows, :]] * (width // 128), axis=1)
        contrib = (o * gate).astype(BF16)
        send[e] = jnp.dot(place, contrib, preferred_element_type=F32).astype(BF16)

    def early(e):
        rows = pl.ds(e * cap, cap)
        up(pk.at[rows, :], cap, e)
        down_copy(e).wait()
        scatter(e, rows)
        for k in range(2, NDEV - 1):
            ret_copy(e, k).start()
        loc_copy(e).start()

    def diagonal(e, carry):
        rows = pl.ds(pl.multiple_of(e * cap, cap), cap)
        m = 2 * slots
        base = pl.multiple_of((dg // 2) * m, m)
        code = code_s[pl.ds(e, 1), :].astype(jnp.int32) - base
        here = jnp.broadcast_to(code, (m, cap)) == _iota((m, cap), 0)
        gate = jnp.sum(jnp.where(here, gate_ref[pl.ds(e, 1), :], 0.0), axis=1, keepdims=True)
        dpk[...] = jnp.dot(_onehot(here), pk[rows, :], preferred_element_type=F32).astype(BF16)
        tile = 1024

        def some(j, c):
            cols = pl.ds(pl.multiple_of(j * tile, tile), tile)
            z = jnp.dot(dpk[...], wup[e % 2, :, cols], preferred_element_type=F32)
            hid[0:m, cols] = _gelu(z).astype(BF16)
            return c

        lax.fori_loop(0, ff // tile, some, 0)
        up_copy(e + 2).start()
        o = jnp.dot(hid[0:m, :], wdn[e % 2], preferred_element_type=F32)
        send[e, pl.ds(base, m), :] = (o * gate).astype(BF16)
        down_copy(e + 2).start()
        for k in range(2):
            ret_copy(e, k).start()
        return carry

    def produce(e):
        rows = pl.ds(pl.multiple_of(e * cap, cap), cap)
        up(pk.at[rows, :], cap, e)

        @pl.when(e + 2 < n_exp)
        def _():
            up_copy(e + 2).start()

        down_copy(e).wait()
        scatter(e, rows)

        @pl.when(e + 2 < n_exp)
        def _():
            down_copy(e + 2).start()

        @pl.when(e < last)
        def _():
            for k in spread:
                ret_copy(e, k).start()
            loc_copy(e).start()

        @pl.when(e == last)
        def _():
            turns = ((2, 0), (0, 0), (4, 0), (0, 1), (3, 0), (1, 0), (5, 0), (1, 1), (2, 1), (4, 1), (3, 1), (5, 1), (6, 0), (6, 1))
            for k, h in turns:
                src, dst = half_refs(peers[k], h)
                remote(src, dst, snd_sem, rcv_sem.at[last + h], peers[k]).start()
            for h in range(2):
                src, dst = half_refs(me, h)
                pltpu.make_async_copy(src, dst, rcv_sem.at[last + h]).start()

    def arrived(e):
        take(ret.at[e], rcv_sem.at[e])

    def adds(e, j, tile):
        row = rowtab[pl.ds(e, 1), :].astype(jnp.int32)
        hot = _onehot(jnp.broadcast_to(row, (tile, nslot)) == _iota((tile, nslot), 0) + j * tile)
        return jnp.dot(hot, ret[e].reshape(nslot, width), preferred_element_type=F32)

    def combine(e):
        arrived(e)
        tile = 256

        def some(j, carry):
            rows = pl.ds(pl.multiple_of(j * tile, tile), tile)
            yacc[rows, :] += adds(e, j, tile)
            return carry

        lax.fori_loop(0, tok // tile, some, 0)

    qb = hb // 2
    gather(me, 0, hb, fresh=True)
    slot(0)
    gather(me, hb, hb)
    slot(1)
    from_sib(0)
    gather(sib, 0, hb)
    slot(2)
    from_sib(1)
    gather(sib, hb, hb)
    slot(3)
    gather(xn, 0, hb)
    from_sib(2)
    slot(4)
    for dev in peers:
        remote(rt_send.at[dev], rt_recv.at[me], rt_snd, rt_sem, dev).start()
    gather(yn, hb, hb)
    gather(xs, 0, hb)
    slot(5)
    from_sib(3)
    gather(ys, hb, hb)
    gather(xn, hb, qb)
    slot(6)
    gather(yn, 0, qb)
    from_sib(4)
    gather(xs, hb, qb)
    gather(ys, 0, qb)
    slot(7)
    first, later = (0, 1), (1, n_exp // 2)

    def third(pairs):
        gather(xn, hb + qb, qb, pairs)
        gather(yn, qb, qb, pairs)
        gather(xs, hb + qb, qb, pairs)
        gather(ys, qb, qb, pairs)

    from_sib(5)
    third(first)
    early(0)
    slot(8)
    early(1)
    slot(9)
    third(later)
    slot(10)
    from_sib(6)
    for dev in (dg, ds):
        gather(dev, 0, qb, first)
        gather(dev, tok - qb, qb, first)
    slot(11)
    from_sib(7)
    for dev in (dg, ds):
        gather(dev, qb, hb, first)

    lax.fori_loop(0, 2, diagonal, 0)

    take(rt_recv.at[pl.ds(0, NDEV - 1)], rt_sem)
    for p in range(NDEV // 2):
        rowtab[:, p * 128 : (p + 1) * 128] = rt_recv[2 * p] + rt_recv[2 * p + 1] - 1.0

    def pair(p, carry):
        for dev in (dg, ds):
            gather(dev, 0, tok, (p, p + 1))
        produce(2 * p)

        @pl.when(p >= 2)
        def _():
            combine(2 * p - 3)

        produce(2 * p + 1)
        combine(2 * p - 2)
        return carry

    lax.fori_loop(1, n_exp // 2, pair, 0)

    def rest(e, carry):
        combine(e)
        return carry

    lax.fori_loop(n_exp - 3, n_exp - 1, rest, 0)
    row = rowtab[pl.ds(last, 1), :].astype(jnp.int32)
    for h in range(2):
        picks_h = [row[:, d * slots + h * hs : d * slots + (h + 1) * hs] for d in range(NDEV)]
        lanes = jnp.concatenate(picks_h, axis=1)
        take(ret.at[last, pl.ds(0, NDEV // 2)], rcv_sem.at[last + h])
        tile = 512
        for j in range(tok // tile):
            rows = pl.ds(j * tile, tile)
            hot = _onehot(jnp.broadcast_to(lanes, (tile, nslot // 2)) == _iota((tile, nslot // 2), 0) + j * tile)
            back = ret[last, :, h * hs : (h + 1) * hs, :].reshape(nslot // 2, width)
            total = yacc[rows, :] + jnp.dot(hot, back, preferred_element_type=F32)
            if h == 0:
                yacc[rows, :] = total
            else:
                y_ref[rows, :] = total.astype(BF16)

    take(xall.at[pl.ds(0, 7)], ag_snd)
    take(rt_send.at[pl.ds(0, NDEV - 1)], rt_snd)
    take(send.at[pl.ds(0, n_exp * (NDEV - 1) // NDEV)], snd_sem)


def solution(mesh):
    def local_layer(x_loc, sel_loc, gate_loc, up_loc, down_loc):
        tok, width = x_loc.shape
        n_exp, cap = sel_loc.shape
        ff = up_loc.shape[2]
        slots = 2 * cap // NDEV
        nslot = NDEV * slots
        dma = pltpu.SemaphoreType.DMA
        vmem = pl.BlockSpec(memory_space=pltpu.VMEM)
        hbm = pl.BlockSpec(memory_space=pl.ANY)
        return pl.pallas_call(
            functools.partial(kernel, slots),
            out_shape=pltpu.VMEM((tok, width), BF16),
            in_specs=[hbm] * 5,
            out_specs=vmem,
            scratch_shapes=[
                pltpu.VMEM((n_exp, cap), jnp.int32),
                pltpu.VMEM((n_exp, cap), F32),
                pltpu.VMEM((NDEV, tok, width), BF16),
                pltpu.VMEM((2, width, ff), BF16),
                pltpu.VMEM((2, ff, width), BF16),
                pltpu.VMEM((n_exp, nslot, width), BF16),
                pltpu.VMEM((n_exp, NDEV, slots, width), BF16),
                pltpu.VMEM((n_exp * cap, width), BF16),
                pltpu.VMEM((cap, ff), BF16),
                pltpu.VMEM((2 * slots, width), BF16),
                pltpu.VMEM((tok, width), F32),
                pltpu.VMEM((n_exp * cap, 128), jnp.int32),
                pltpu.VMEM((n_exp * cap, 128), F32),
                pltpu.VMEM((n_exp, cap), F32),
                pltpu.VMEM((NDEV, n_exp, 128), F32),
                pltpu.VMEM((NDEV, n_exp, 128), F32),
                pltpu.VMEM((n_exp, nslot), F32),
                dma((3,)),
                dma((2,)),
                dma((2,)),
                dma,
                dma((CHUNKS + CHUNKS // 2,)),
                dma((8,)),
                dma,
                dma,
                dma,
                dma((n_exp + 1,)),
            ],
            compiler_params=pltpu.CompilerParams(
                collective_id=0, has_side_effects=True, vmem_limit_bytes=64_000_000
            ),
            name="moe",
        )(x_loc, sel_loc, gate_loc, up_loc, down_loc)

    row_spec = P(("dp", "ep"), None)
    weight_spec = P("ep", None, None)
    return jax.shard_map(
        local_layer,
        mesh=mesh,
        in_specs=(row_spec, row_spec, row_spec, weight_spec, weight_spec),
        out_specs=row_spec,
        check_vma=False,
    )
```
